128 devices in a mesh: gx: 8 (over y, core), gy: 16 (over x, z).
Axes of the slice: x: 4, y: 4, z: 4, core: 2. Of those that a mesh axis runs over, the one named last changes fastest.
Arguments:
- disp: float32 [3, 64, 256, 128], P(None, 'gx', 'gy'), may hold values from -3 to 3
- vel: float32 [3, 64, 256, 128], P(None, 'gx', 'gy'), may hold values from -30 to 30
- load: float32 [3, 64, 256, 128], P(None, 'gx', 'gy'), may hold values from -96 to 96
- flags: int32 [64, 256, 128], P('gx', 'gy'), may hold values 0 or 1
- mask_bits: int32 [4, 64, 256, 128], P(None, 'gx', 'gy'), may hold values from 0 to 2147483647, as said below
Outputs:
- disp_out: float32 [3, 64, 256, 128], P(None, 'gx', 'gy')
- vel_out: float32 [3, 64, 256, 128], P(None, 'gx', 'gy')
The draws below stay inside these ranges and needn't reach their ends.
Inputs may be any that keep to these rules, and one draw needn't show every extreme that they name: `mask_bits`: bit b (0 to 30) of word w marks the cell's bond to neighbour number 31 w + b as broken; bit 31, and bits of numbers 122 and above, are zero.
All inputs are finite; a program needn't handle non-finite values. No bound on the sum of `flags` on one device may be relied on, other than what follows from the above.
Results may differ from the reference program's by a relative error of at most 0.0001.
Values sent between devices are 32-bit elements; how exact they have to be, the bound alone decides.
A program may use at most 128 MiB of HBM per device.

```python
import math
import jax
import jax.numpy as jnp
from jax import lax

NZ = 128
ITERS = 8
NX = 64
NY = 256


def neighbour_table_drawn():
    table = []
    for across in range(-3, 4):
        for along in range(-3, 4):
            for upward in range(-3, 4):
                length = across * across + along * along + upward * upward
                if 0 < length <= 9:
                    table.append((across, along, upward))
    return table


def draw_vel(key, part):
    places_x = jnp.arange(NX, dtype=jnp.float32) / max(NX - 1, 1)
    places_y = jnp.arange(NY, dtype=jnp.float32) / max(NY - 1, 1)
    amplitude = 0.3 * (1.0 + 2.0 * places_x)[:, None, None] * (1.0 + 2.0 * places_y)[None, :, None]
    first = jax.random.fold_in(key, 11)
    base = jnp.clip(jax.random.normal(first, (3, NX, NY, NZ), jnp.float32), -4.0, 4.0)
    return (amplitude[None] * base).astype(jnp.float32)


def draw_mask_bits(key, part):
    table = neighbour_table_drawn()
    places_x = jnp.arange(NX, dtype=jnp.int32)[:, None, None]
    places_y = jnp.arange(NY, dtype=jnp.int32)[None, :, None]
    middle = NX // 2
    words = []
    for word in range(4):
        packed = jnp.zeros((NX, NY, NZ), jnp.int32)
        for bit in range(31):
            number = 31 * word + bit
            if number < 122:
                across = table[number][0]
                coin = jax.random.randint(jax.random.fold_in(key, 100 + number), (NX, NY, NZ), 0, 16)
                crosses = (places_x < middle) & (places_x + across >= middle) | (places_x >= middle) & (places_x + across < middle)
                crack = crosses & (places_y < NY // 2)
                broken = (coin == 0) | crack
                packed = packed | broken.astype(jnp.int32) << bit
        words.append(packed)
    return jnp.stack(words)


def set_ends(array, rng, low, high):
    index_at = [jax.random.randint(jax.random.fold_in(rng, axis), (), 0, length) for axis, length in enumerate(array.shape)]
    widest = array.shape.index(max(array.shape))
    next_to = index_at[:widest] + [(index_at[widest] + 1) % array.shape[widest]] + index_at[widest + 1:]
    return array.at[tuple(index_at)].set(low).at[tuple(next_to)].set(high)


def level_of(rng, dims, split, low, high):
    factor_of = 1.0
    for dim, shards_of in split:
        steps = jax.random.uniform(jax.random.fold_in(jax.random.fold_in(rng, 6), dim), (shards_of,), jnp.float32, low / len(split), high / len(split))
        factor_of = factor_of * jnp.repeat(jnp.exp(steps), dims[dim] // shards_of).reshape((-1,) + (1,) * (len(dims) - 1 - dim))
    return factor_of


def scatter_about(own_key, dims, spread, bound, split=(), kind=jnp.bfloat16):
    factor_of = level_of(own_key, dims, split, -0.22, 0.18) if split else 1.0
    entries = jax.random.normal(own_key, dims, jnp.float32) * spread * factor_of
    return jnp.minimum(jnp.maximum(entries, -bound), bound).astype(kind)


def setup_inputs(seed: int = 0) -> dict:
    key_of = jax.random.split(jax.random.key(seed), 6)
    return {
        "disp": scatter_about(key_of[0], (3, NX, NY, NZ), 0.5, 3.0, ((1, 8), (2, 16)), jnp.float32),
        "vel": draw_vel(jax.random.fold_in(key_of[5], 71), 0),
        "load": scatter_about(key_of[2], (3, NX, NY, NZ), 16.0, 96.0, ((1, 8), (2, 16)), jnp.float32),
        "flags": set_ends((jax.random.randint(key_of[3], (NX, NY, NZ), 0, 3) < 1).astype(jnp.int32), jax.random.fold_in(key_of[3], 1), 0, 1),
        "mask_bits": draw_mask_bits(jax.random.fold_in(key_of[5], 71), 0),
    }


fictive_mass = 64.0
epsilon = 1e-06

def neighbour_table():
    table = []
    for across in range(-3, 4):
        for along in range(-3, 4):
            for upward in range(-3, 4):
                length = across * across + along * along + upward * upward
                if 0 < length <= 9:
                    table.append((across, along, upward))
    return table

def bond_forces(field_pad, words, words_pad, exist_pad):
    rows = words.shape[1]
    cols = words.shape[2]
    depth = words.shape[3]
    centre = field_pad[:, 3:3 + rows, 3:3 + cols, 3:3 + depth]
    totals = [jnp.zeros((rows, cols, depth), jnp.float32) for index in range(3)]
    for number, offset in enumerate(neighbour_table()):
        across, along, upward = offset
        word, bit = divmod(number, 31)
        mirror_word, mirror_bit = divmod(121 - number, 31)
        window = (slice(3 + across, 3 + across + rows), slice(3 + along, 3 + along + cols), slice(3 + upward, 3 + upward + depth))
        other = field_pad[(slice(None),) + window]
        own_flag = words[word] >> bit & 1
        far_flag = words_pad[mirror_word][window] >> mirror_bit & 1
        intact = (own_flag | far_flag == 0) & (exist_pad[window] > 0)
        length = float(across * across + along * along + upward * upward)
        weight = 1.0 / (length * math.sqrt(length))
        stretch = float(across) * (other[0] - centre[0]) + float(along) * (other[1] - centre[1]) + float(upward) * (other[2] - centre[2])
        scaled = jnp.where(intact, stretch * weight, jnp.float32(0.0))
        totals[0] = totals[0] + float(across) * scaled
        totals[1] = totals[1] + float(along) * scaled
        totals[2] = totals[2] + float(upward) * scaled
    return jnp.stack(totals)

def reference(disp, vel, load, flags, mask_bits):
    words_pad = jnp.pad(mask_bits, ((0, 0), (3, 3), (3, 3), (3, 3)))
    exist_pad = jnp.pad(jnp.ones(mask_bits.shape[1:], jnp.int32), 3)
    applied = flags.astype(jnp.float32)[None] * load
    count = 3.0 * NX * NY * NZ

    def internal(field):
        field_pad = jnp.pad(field, ((0, 0), (3, 3), (3, 3), (3, 3)))
        return bond_forces(field_pad, mask_bits, words_pad, exist_pad)
    previous = lax.fori_loop(0, 1, lambda index, carry: internal(disp - vel), jnp.zeros_like(disp))

    def relax(index, state):
        field, speed, before = state
        current = internal(field)
        total = current + applied
        kinetic = jnp.sum(speed * speed)
        rayleigh = jnp.sum(speed * (before - current))
        damping = 2.0 * jnp.sqrt(rayleigh / count / (fictive_mass * (kinetic / count + epsilon)))
        alpha = (2.0 - damping) / (2.0 + damping)
        beta = 2.0 / (fictive_mass * (2.0 + damping))
        speed = alpha * speed + beta * total
        return (field + speed, speed, current)
    field, speed, before = lax.fori_loop(0, ITERS, relax, (disp, vel, previous))
    return (field, speed)
```

```python
import functools
import math

import jax
import jax.numpy as jnp
from jax import lax
from jax.experimental import pallas as pl
from jax.experimental.pallas import tpu as pltpu
from jax.sharding import PartitionSpec as P

ITERS = 8
MASS = 64.0
EPSILON = 1e-06
ROWS = 8
COLS = 16
DEPTH = 128
PAD = 8
WIDE = COLS + 2 * PAD
TALL = ROWS + 6
GROUP = 4
SLOTS = 4
F32 = jnp.float32
I32 = jnp.int32


def neighbour_table():
    table = []
    for across in range(-3, 4):
        for along in range(-3, 4):
            for upward in range(-3, 4):
                length = across * across + along * along + upward * upward
                if 0 < length <= 9:
                    table.append((across, along, upward))
    return table


TABLE = neighbour_table()
NUMBER = {offset: k for k, offset in enumerate(TABLE)}
BONDS = len(TABLE)


def on_axis(offset):
    return sum(1 for part in offset if part) == 1


def weight_of(offset):
    length = float(sum(part * part for part in offset))
    weight = 1.0 / (length * math.sqrt(length))
    return weight * length if on_axis(offset) else weight


def oblique(b, c):
    return [a for a in range(-2, 3) if (a, b, c) in NUMBER and not on_axis((a, b, c))]


EDGE = []
for _c in range(-2, 3):
    for _reach in (1, 2, 3):
        for _a in range(-2, 3):
            if (_a, _reach, _c) in NUMBER:
                for _j in range(_reach):
                    EDGE.append((_a, _reach, _c, _j, _reach - 1 - _j))
EDGE_AT = {entry[:4]: n for n, entry in enumerate(EDGE)}


def add(total, term):
    return term if total is None else total + term


def sub(total, term):
    return -term if total is None else total - term


def scaled(factor, value):
    if factor == 1:
        return value
    if factor == -1:
        return -value
    return float(factor) * value


def plus_scaled(total, factor, value):
    if total is None:
        return scaled(factor, value)
    if factor == 1:
        return total + value
    if factor == -1:
        return total - value
    return total + float(factor) * value


def combine(weights, totals):
    out = None
    for factor, value in zip(weights, totals):
        if factor and value is not None:
            out = plus_scaled(out, factor, value)
    return out


def turned(value, c):
    if c == 0:
        return value
    return pltpu.roll(value, (-c) % DEPTH, 1)


def moments(terms):
    zeroth = None
    for a in sorted(terms):
        zeroth = add(zeroth, terms[a])
    first = None
    if 2 in terms:
        first = add(first, terms[2])
    if -2 in terms:
        first = sub(first, terms[-2])
    if first is not None:
        first = 2.0 * first
    if 1 in terms:
        first = add(first, terms[1])
    if -1 in terms:
        first = sub(first, terms[-1])
    return zeroth, first


def local_pass(slot, field, bond, diag, out):
    def group(g, carry):
        base = g * GROUP
        for t in range(2):
            col = PAD + 8 * t

            def coef(offset, i):
                start = pl.multiple_of((base + i) * COLS + 8 * t, 8)
                return bond[NUMBER[offset], pl.ds(start, 8), :]

            def source(part, i, b):
                return field[slot, part, base + 3 + i, pl.ds(col + b, 8), :]

            for c in (0, 1, -1, 2, -2, 3, -3):
                g0 = [None] * GROUP
                g1 = [None] * GROUP
                g2 = [None] * GROUP
                if c:
                    for i in range(GROUP):
                        g2[i] = coef((0, 0, c), i) * source(2, i, 0)
                if c == 0:
                    for i in range(GROUP):
                        for a in (1, -1, 2, -2, 3, -3):
                            g0[i] = add(g0[i], coef((a, 0, 0), i) * source(0, i + a, 0))
                        for b in (1, -1, 2, -2, 3, -3):
                            g1[i] = add(g1[i], coef((0, b, 0), i) * source(1, i, b))
                if abs(c) < 3:
                    n0 = [None] * GROUP
                    n1 = [None] * GROUP
                    for b in (2, -2, 1, -1, 0):
                        reach = oblique(b, c)
                        if not reach:
                            continue
                        span = range(min(reach), GROUP + max(reach))
                        u0 = {i: source(0, i, b) for i in span}
                        twice = {i: 2.0 * u0[i] for i in span} if 2 in reach else None
                        u1 = {i: source(1, i, b) if b else None for i in span}
                        u2 = {i: source(2, i, b) if c else None for i in span}
                        s = {i: combine((b, c), (u1[i], u2[i])) for i in span}
                        for i in range(GROUP):
                            terms = {}
                            for a in reach:
                                near = s[i + a]
                                if abs(a) == 1:
                                    near = near + u0[i + a] if a > 0 else near - u0[i + a]
                                elif a:
                                    near = near + twice[i + a] if a > 0 else near - twice[i + a]
                                terms[a] = coef((a, b, c), i) * near
                            zeroth, first = moments(terms)
                            g0[i] = add(g0[i], first)
                            if c:
                                n0[i] = add(n0[i], zeroth)
                            if b == 2:
                                n1[i] = zeroth
                            elif b == -2:
                                n1[i] = 2.0 * (n1[i] - zeroth)
                            elif b:
                                n1[i] = plus_scaled(n1[i], b, zeroth)
                    for i in range(GROUP):
                        g1[i] = add(g1[i], n1[i])
                        if c:
                            g2[i] = plus_scaled(g2[i], c, n0[i])
                for i in range(GROUP):
                    for part, value in enumerate((g0[i], g1[i], g2[i])):
                        if c == 0:
                            u = [source(other, i, 0) for other in range(3)]
                            own = None
                            for other in range(3):
                                pair = DIAG[min(part, other), max(part, other)]
                                own = add(own, diag[pair, base + i, pl.ds(8 * t, 8), :] * u[other])
                            value = -own if value is None else value - own
                            out[part, base + i, pl.ds(8 * t, 8), :] = value
                        elif value is not None:
                            out[part, base + i, pl.ds(8 * t, 8), :] += turned(value, c)
        return carry

    lax.fori_loop(0, ROWS // GROUP, group, 0)


DIAG = {(0, 0): 0, (0, 1): 1, (1, 1): 2, (0, 2): 3, (1, 2): 4, (2, 2): 5}


def across_pass(slot, near, far, bond, out):
    for side in range(2):
        sign = 1 if side else -1
        edge = ROWS - 1 if side else 0
        for t in range(2):
            col = PAD + 8 * t

            def coef(offset, i):
                return bond[NUMBER[offset], pl.ds((edge - sign * i) * COLS + 8 * t, 8), :]

            def source(part, layer, b):
                e = layer if side else 1 - layer
                return near[slot, side, part, e, pl.ds(col + b, 8), :]

            sums = [[None] * 3 for i in range(2)]
            third = None
            for c in (0, 1, -1, 2, -2):
                g = [[None] * 3 for i in range(2)]
                if c == 0:
                    for layer in range(2):
                        u0 = source(0, layer, 0)
                        for i in range(3):
                            a = sign * (i + layer + 1)
                            if abs(a) <= 3:
                                term = coef((a, 0, 0), i) * u0
                                if i < 2:
                                    g[i][0] = add(g[i][0], term)
                                else:
                                    third = term
                    g[0][0] = g[0][0] + coef((3 * sign, 0, 0), 0) * far[slot, side, pl.ds(col, 8), :]
                n0 = [None] * 2
                n1 = [None] * 2
                for b in (2, -2, 1, -1, 0):
                    reach = oblique(b, c)
                    if not reach:
                        continue
                    zeroth = [None] * 2
                    deep = [None] * 2
                    for layer in range(max(reach)):
                        u0 = source(0, layer, b)
                        u1 = source(1, layer, b) if b else None
                        u2 = source(2, layer, b) if c else None
                        s = combine((b, c), (u1, u2))
                        for i in range(2):
                            size = i + layer + 1
                            a = sign * size
                            if a in reach:
                                q = plus_scaled(s, a, u0)
                                term = coef((a, b, c), i) * q
                                zeroth[i] = add(zeroth[i], term)
                                if size == 1:
                                    g[i][0] = plus_scaled(g[i][0], sign, term)
                                else:
                                    deep[i] = add(deep[i], term)
                    for i in range(2):
                        if deep[i] is not None:
                            g[i][0] = plus_scaled(g[i][0], 2 * sign, deep[i])
                        if zeroth[i] is None:
                            continue
                        if c:
                            n0[i] = add(n0[i], zeroth[i])
                        if b:
                            n1[i] = plus_scaled(n1[i], b, zeroth[i])
                for i in range(2):
                    g[i][1] = n1[i]
                    g[i][2] = scaled(c, n0[i]) if c else None
                    for part in range(3):
                        if g[i][part] is not None:
                            sums[i][part] = add(sums[i][part], turned(g[i][part], c))
            for i in range(2):
                row = edge - sign * i
                for part in range(3):
                    out[part, row, pl.ds(8 * t, 8), :] += sums[i][part]
            out[0, edge - 2 * sign, pl.ds(8 * t, 8), :] += third


def along_pass(slot, rim, bond_edge, out):
    for side in range(2):
        sign = 1 if side else -1
        edge = COLS - 1 if side else 0

        def coef(a, size, c, j):
            return bond_edge[side, EDGE_AT[a, size, c, j]]

        def source(part, layer, a):
            return rim[slot, side, part * 2 + layer, pl.ds(8 + a, 8), :]

        sums = [[None] * 3 for j in range(2)]
        third = None
        for c in (0, 1, -1, 2, -2):
            g = [[None] * 3 for j in range(2)]
            if c == 0:
                for layer in range(3):
                    at = 6 if layer == 2 else 2 + layer
                    u1 = rim[slot, side, at, pl.ds(8, 8), :]
                    for j in range(3 - layer):
                        term = coef(0, layer + 1 + j, 0, j) * u1
                        if j < 2:
                            g[j][1] = add(g[j][1], term)
                        else:
                            third = term
            n0 = [None] * 2
            n1 = [None] * 2
            for a in (2, -2, 1, -1, 0):
                reach = [size for size in (1, 2) if (a, size, c) in NUMBER and not on_axis((a, size, c))]
                if not reach:
                    continue
                zeroth = [None] * 2
                deep = [None] * 2
                for layer in range(max(reach)):
                    u0 = source(0, layer, a) if a else None
                    u1 = source(1, layer, a)
                    u2 = source(2, layer, a) if c else None
                    s = combine((a, c), (u0, u2))
                    for j in range(2):
                        size = j + layer + 1
                        if size in reach:
                            term = coef(a, size, c, j) * plus_scaled(s, sign * size, u1)
                            zeroth[j] = add(zeroth[j], term)
                            if size == 1:
                                g[j][1] = plus_scaled(g[j][1], sign, term)
                            else:
                                deep[j] = add(deep[j], term)
                for j in range(2):
                    if deep[j] is not None:
                        g[j][1] = plus_scaled(g[j][1], 2 * sign, deep[j])
                    if zeroth[j] is None:
                        continue
                    if c:
                        n0[j] = add(n0[j], zeroth[j])
                    if a:
                        n1[j] = plus_scaled(n1[j], a, zeroth[j])
            for j in range(2):
                g[j][0] = n1[j]
                g[j][2] = scaled(c, n0[j]) if c else None
                for part in range(3):
                    if g[j][part] is not None:
                        sums[j][part] = add(sums[j][part], turned(g[j][part], c))
        for r in range(ROWS):
            for j in range(2):
                at = edge - sign * j
                for part in range(3):
                    out[part, r, at : at + 1, :] += sums[j][part][r : r + 1, :]
            at = edge - 2 * sign
            out[1, r, at : at + 1, :] += third[r : r + 1, :]


def build_bonds(words, bond, diag):
    def row(r, carry):
        lane = lax.broadcasted_iota(I32, (8, DEPTH), 1)
        for t in range(2):
            start = pl.multiple_of(r * COLS + 8 * t, 8)
            own = [words[w, r + 3, pl.ds(PAD + 8 * t, 8), :] for w in range(4)]
            totals = [None] * 6
            for c in range(-3, 4):
                if c:
                    outside = lane < c if c > 0 else lane >= DEPTH + c
                    near = [jnp.where(outside, I32(-1), pltpu.roll(own[w], c % DEPTH, 1)) for w in range(4)]
                else:
                    near = own
                sums = [None] * 6
                for b in range(-3, 4):
                    values = {}
                    for a in range(-3, 4):
                        k = NUMBER.get((a, b, c))
                        if k is None:
                            continue
                        word, bit = divmod(k, 31)
                        far_word, far_bit = divmod(BONDS - 1 - k, 31)
                        far = words[far_word, r + 3 + a, pl.ds(PAD + 8 * t + b, 8), :]
                        broken = (near[word] & I32(1 << bit)) | (far & I32(1 << far_bit))
                        value = jnp.where(broken == 0, F32(weight_of((a, b, c))), F32(0.0))
                        bond[k, pl.ds(start, 8), :] = value
                        if on_axis((a, b, c)):
                            at = 0 if a else (2 if b else 5)
                            sums[at] = add(sums[at], value)
                        else:
                            values[a] = value
                    if not values:
                        continue
                    zeroth, first = moments(values)
                    second = None
                    if 2 in values:
                        second = 4.0 * (values[2] + values[-2])
                    second = add(second, values[1] + values[-1])
                    sums[0] = add(sums[0], second)
                    if b:
                        sums[1] = plus_scaled(sums[1], b, first)
                        sums[2] = plus_scaled(sums[2], b * b, zeroth)
                    if c:
                        sums[3] = plus_scaled(sums[3], c, first)
                        sums[5] = plus_scaled(sums[5], c * c, zeroth)
                        if b:
                            sums[4] = plus_scaled(sums[4], b * c, zeroth)
                for n in range(6):
                    if sums[n] is not None:
                        totals[n] = add(totals[n], turned(sums[n], c))
            for n in range(6):
                diag[n, r, pl.ds(8 * t, 8), :] = totals[n]
        return carry

    lax.fori_loop(0, ROWS, row, 0)


def gather_edges(bond, bond_edge):
    for side in range(2):
        sign = 1 if side else -1
        edge = COLS - 1 if side else 0
        for n, (a, size, c, j, layer) in enumerate(EDGE):
            k = NUMBER[a, sign * size, c]
            bond_edge[side, n] = bond[k, pl.ds(edge - sign * j, ROWS, stride=COLS), :]


def kernel(
    nx, ny,
    disp, vel, load, flags, mask,
    u_out, v_out,
    field, near, far, rim, corner, rim_send, corner_send,
    words, words_rim, words_corner, words_rim_send, words_corner_send,
    bond, bond_edge, diag,
    force, state, keep, load_buf, flag_buf,
    ring_one, ring_two,
    in_sem, send_sem, recv_sem, word_send, word_recv, sum_send, sum_recv,
):
    rate, total, pull = state.at[0], state.at[1], keep.at[0]
    ax = lax.axis_index("gx")
    ay = lax.axis_index("gy")
    here = {-1: (ax > 0, ay > 0), 1: (ax < nx - 1, ay < ny - 1)}

    def exists(dx, dy):
        cond = None
        if dx:
            cond = here[dx][0]
        if dy:
            other = here[dy][1]
            cond = other if cond is None else cond & other
        return cond

    def device(dx, dy):
        return {"gx": ax + dx, "gy": ay + dy}

    sides = [(dx, dy) for dx in (-1, 0, 1) for dy in (-1, 0, 1) if dx or dy]
    diagonals = [(dx, dy) for dx, dy in sides if dx and dy]

    own_rows = pl.ds(3, ROWS)
    own_cols = pl.ds(PAD, COLS)
    loads = [
        pltpu.make_async_copy(disp, field.at[1, :, own_rows, own_cols], in_sem.at[0]),
        pltpu.make_async_copy(vel, field.at[0, :, own_rows, own_cols], in_sem.at[1]),
        pltpu.make_async_copy(mask, words.at[:, own_rows, own_cols], in_sem.at[2]),
        pltpu.make_async_copy(disp, u_out, in_sem.at[3]),
        pltpu.make_async_copy(vel, v_out, in_sem.at[4]),
        pltpu.make_async_copy(load, load_buf, in_sem.at[5]),
        pltpu.make_async_copy(flags, flag_buf, in_sem.at[6]),
    ]
    for copy in loads:
        copy.start()

    zero8 = jnp.zeros((8, DEPTH), F32)

    near[...] = jnp.zeros(near.shape, F32)
    far[...] = jnp.zeros(far.shape, F32)
    rim[...] = jnp.zeros(rim.shape, F32)
    words_rim[...] = jnp.full(words_rim.shape, -1, I32)
    words_corner[...] = jnp.full(words_corner.shape, -1, I32)
    for w in range(4):
        for r in list(range(3)) + list(range(TALL - 3, TALL)):
            words[w, r] = jnp.full((WIDE, DEPTH), -1, I32)

    barrier = pltpu.get_barrier_semaphore()
    for step in range(1, nx):
        pl.semaphore_signal(barrier, inc=1, device_id={"gx": lax.rem(ax + step, nx), "gy": ay})
    for step in range(1, ny):
        pl.semaphore_signal(barrier, inc=1, device_id={"gx": ax, "gy": lax.rem(ay + step, ny)})
    for dx, dy in diagonals:
        where = {"gx": lax.rem(ax + dx + nx, nx), "gy": lax.rem(ay + dy + ny, ny)}
        pl.semaphore_signal(barrier, inc=1, device_id=where)

    def clear(slot, carry):
        for part in range(3):
            for r in list(range(3)) + list(range(TALL - 3, TALL)):
                field[slot, part, r] = jnp.zeros((WIDE, DEPTH), F32)
            for r in range(3, TALL - 3):
                field[slot, part, r, 0:PAD, :] = zero8
                field[slot, part, r, PAD + COLS : WIDE, :] = zero8
        return carry

    lax.fori_loop(0, SLOTS, clear, 0)

    pl.semaphore_wait(barrier, nx + ny + 2)

    def edge_rows(dx):
        return (0, 2) if dx < 0 else (ROWS - 2, ROWS - 3)

    def halo_copies(slot, dx, dy):
        into = {-1: 1, 1: 0}
        if dx and dy:
            n = into[dx] * 2 + into[dy]
            return [(corner_send.at[slot, n], corner.at[slot, n], 6 + n)]
        if dx:
            first, third = edge_rows(dx)
            side = into[dx]
            return [
                (
                    field.at[slot, :, pl.ds(3 + first, 2), own_cols],
                    near.at[slot, side, :, :, own_cols],
                    side,
                ),
                (field.at[slot, 0, 3 + third, own_cols], far.at[slot, side, own_cols], 2 + side),
            ]
        side = into[dy]
        return [(rim_send.at[slot, side], rim.at[slot, side, :, pl.ds(8, 8)], 4 + side)]

    def halo_send(slot):
        for side in range(2):
            for part in range(3):
                for layer in range(3 if part == 1 else 2):
                    at = 6 if layer == 2 else part * 2 + layer
                    col = PAD + (layer if side else COLS - 1 - layer)
                    for r in range(ROWS):
                        rim_send[slot, side, at, r : r + 1, :] = field[slot, part, 3 + r, col : col + 1, :]
        for dx, dy in sides:
            if not (dx and dy):
                send_all(slot, dx, dy)
        for dx, dy in diagonals:
            n = (1 if dx < 0 else 0) * 2 + (1 if dy < 0 else 0)
            row = 3 + (0 if dx < 0 else ROWS - 2)
            col = PAD + (0 if dy < 0 else COLS - 2)
            for part in range(3):
                for e in range(2):
                    at = (part * 2 + e) * 2
                    corner_send[slot, n, at : at + 2, :] = field[slot, part, row + e, col : col + 2, :]
        for dx, dy in diagonals:
            send_all(slot, dx, dy)

    def send_all(slot, dx, dy):
        @pl.when(exists(dx, dy))
        def _():
            for src, dst, n in halo_copies(slot, dx, dy):
                pltpu.make_async_remote_copy(
                    src_ref=src, dst_ref=dst, send_sem=send_sem.at[slot, n], recv_sem=recv_sem.at[slot, n],
                    device_id=device(dx, dy),
                ).start()

    def halo_wait(slot):
        for dx, dy in sides:
            @pl.when(exists(dx, dy))
            def _():
                for src, dst, n in halo_copies(slot, dx, dy):
                    pltpu.make_async_remote_copy(
                        src_ref=src, dst_ref=dst, send_sem=send_sem.at[slot, n], recv_sem=recv_sem.at[slot, n],
                        device_id=device(dx, dy),
                    ).wait_send()
                for src, dst, n in halo_copies(slot, -dx, -dy):
                    pltpu.make_async_remote_copy(
                        src_ref=src, dst_ref=dst, send_sem=send_sem.at[slot, n], recv_sem=recv_sem.at[slot, n],
                        device_id=device(dx, dy),
                    ).wait_recv()
        for dx, dy in diagonals:
            sx, sy = (1 if dx > 0 else 0), (1 if dy > 0 else 0)
            at = PAD + COLS if sy else PAD - 2

            @pl.when(exists(dx, dy))
            def _():
                for part in range(3):
                    for e in range(2):
                        n = (part * 2 + e) * 2
                        near[slot, sx, part, e, at : at + 2, :] = corner[slot, sx * 2 + sy, n : n + 2, :]

    def word_copies(dx, dy):
        into = {-1: 1, 1: 0}
        if dx and dy:
            n = into[dx] * 2 + into[dy]
            return [(words_corner_send.at[n], words_corner.at[n], 4 + n)]
        if dx:
            first = 3 if dx < 0 else ROWS
            to = TALL - 3 if dx < 0 else 0
            return [(words.at[:, pl.ds(first, 3), own_cols], words.at[:, pl.ds(to, 3), own_cols], into[dx])]
        side = into[dy]
        return [(words_rim_send.at[side], words_rim.at[side], 2 + side)]

    def word_copy(dx, dy, src, dst, n):
        return pltpu.make_async_remote_copy(
            src_ref=src, dst_ref=dst, send_sem=word_send.at[n], recv_sem=word_recv.at[n], device_id=device(dx, dy),
        )

    for copy in (loads[0], loads[1]):
        copy.wait()
    halo_send(0)
    halo_send(1)
    loads[2].wait()
    for side in range(2):
        for w in range(4):
            for layer in range(3):
                col = PAD + (layer if side else COLS - 1 - layer)
                for r in range(ROWS):
                    words_rim_send[side, w, layer, r : r + 1, :] = words[w, 3 + r, col : col + 1, :]
    for dx, dy in diagonals:
        n = (1 if dx < 0 else 0) * 2 + (1 if dy < 0 else 0)
        row = 3 + (0 if dx < 0 else ROWS - 2)
        col = PAD + (0 if dy < 0 else COLS - 2)
        for w in range(4):
            for e in range(2):
                at = (w * 2 + e) * 2
                words_corner_send[n, at : at + 2, :] = words[w, row + e, col : col + 2, :]
    for dx, dy in sides:
        @pl.when(exists(dx, dy))
        def _():
            for src, dst, n in word_copies(dx, dy):
                word_copy(dx, dy, src, dst, n).start()
    for dx, dy in sides:
        @pl.when(exists(dx, dy))
        def _():
            for src, dst, n in word_copies(dx, dy):
                word_copy(dx, dy, src, dst, n).wait_send()
            for src, dst, n in word_copies(-dx, -dy):
                word_copy(dx, dy, src, dst, n).wait_recv()
    for side in range(2):
        for w in range(4):
            for layer in range(3):
                col = PAD + (COLS + layer if side else -1 - layer)
                for r in range(ROWS):
                    words[w, 3 + r, col : col + 1, :] = words_rim[side, w, layer, r : r + 1, :]
    for sx in range(2):
        for sy in range(2):
            row = 3 + (ROWS if sx else -2)
            col = PAD + (COLS if sy else -2)
            for w in range(4):
                for e in range(2):
                    at = (w * 2 + e) * 2
                    words[w, row + e, col : col + 2, :] = words_corner[sx * 2 + sy, at : at + 2, :]

    build_bonds(words, bond, diag)
    gather_edges(bond, bond_edge)

    def sum_copy(src, dst, which, turn, where):
        return pltpu.make_async_remote_copy(
            src_ref=src, dst_ref=dst, send_sem=sum_send.at[which, turn], recv_sem=sum_recv.at[which, turn],
            device_id=where,
        )

    def sum_begin(turn, rows):
        slab = jnp.concatenate([jnp.sum(row, axis=0, keepdims=True) for row in rows] + [jnp.zeros((2, DEPTH), F32)], axis=0)
        ring_one[turn, ax] = slab
        for step in range(1, nx):
            sum_copy(
                ring_one.at[turn, ax], ring_one.at[turn, ax], 0, turn, {"gx": lax.rem(ax + step, nx), "gy": ay}
            ).start()

    def sum_middle(turn):
        some = ring_one.at[turn, pl.ds(0, nx - 1)]
        copy = sum_copy(some, some, 0, turn, {"gx": ax, "gy": ay})
        copy.wait_recv()
        copy.wait_send()
        slab = ring_one[turn, 0]
        for n in range(1, nx):
            slab = slab + ring_one[turn, n]
        ring_two[turn, ay] = slab
        for step in range(1, ny):
            sum_copy(
                ring_two.at[turn, ay], ring_two.at[turn, ay], 1, turn, {"gx": ax, "gy": lax.rem(ay + step, ny)}
            ).start()

    def sum_end(turn):
        some = ring_two.at[turn, pl.ds(0, ny - 1)]
        copy = sum_copy(some, some, 1, turn, {"gx": ax, "gy": ay})
        copy.wait_recv()
        copy.wait_send()
        slab = ring_two[turn, 0]
        for n in range(1, ny):
            slab = slab + ring_two[turn, n]
        sums = jnp.broadcast_to(jnp.sum(slab, axis=1, keepdims=True), (8, DEPTH))
        return [jnp.broadcast_to(sums[n : n + 1, :], (8, DEPTH)) for n in range(6)]

    count = 3.0 * ROWS * nx * COLS * ny * DEPTH

    def damping_of(turn, alpha, beta):
        g0, g1, g2, h0, h1, h2 = sum_end(turn)
        kinetic = alpha * alpha * g0 + 2.0 * alpha * beta * g1 + beta * beta * g2
        rayleigh = -(alpha * alpha * h0 + alpha * beta * h1 + beta * beta * h2)
        rayleigh = jnp.maximum(rayleigh, 0.0)
        damping = 2.0 * jnp.sqrt((rayleigh / count) / (MASS * (kinetic / count + EPSILON)))
        return (2.0 - damping) / (2.0 + damping), 2.0 / (MASS * (2.0 + damping))

    def own(ref_slot, part, r, t):
        return field[ref_slot, part, 3 + r, pl.ds(PAD + 8 * t, 8), :]

    vregs = [(part, r, t) for part in range(3) for r in range(ROWS) for t in range(2)]

    def products(turn, slot, first):
        def body(r, carry):
            acc = list(carry)
            for part in range(3):
                for t in range(2):
                    at = (part, r, pl.ds(8 * t, 8), slice(None))
                    v, w = v_out[at], rate[at]
                    acc[0] += v * v
                    acc[3] += v * w
                    if not first:
                        tt, y = total[at], own(slot, part, r, t)
                        acc[1] += v * tt
                        acc[2] += tt * tt
                        acc[4] += v * y + tt * w
                        acc[5] += tt * y
            return tuple(acc)

        sum_begin(turn, lax.fori_loop(0, ROWS, body, (zero8,) * 6))

    def forces(slot):
        local_pass(slot, field, bond, diag, force)
        halo_wait(slot)
        across_pass(slot, near, far, bond, force)
        along_pass(slot, rim, bond_edge, force)

    for copy in loads[3:]:
        copy.wait()

    def first(n, carry):
        forces(n)
        loaded = n.astype(F32)

        def put(r, carry):
            for t in range(2):
                at = (r, pl.ds(8 * t, 8), slice(None))
                active = loaded * flag_buf[at].astype(F32)
                for part in range(3):
                    value = force[(part,) + at] + active * load_buf[(part,) + at]
                    state[(n, part) + at] = value
                    field[3 - n, part, 3 + r, pl.ds(PAD + 8 * t, 8), :] = value
            return carry

        lax.fori_loop(0, ROWS, put, 0)
        halo_send(3 - n)
        return carry

    lax.fori_loop(0, 2, first, 0)
    products(0, 0, True)

    def second(n, carry):
        forces(3 - n)

        def put(r, carry):
            for part in range(3):
                for t in range(2):
                    at = (part, r, pl.ds(8 * t, 8), slice(None))
                    value = force[at]
                    keep[(n,) + at] = value
                    field[0, part, 3 + r, pl.ds(PAD + 8 * t, 8), :] = value
            return carry

        lax.fori_loop(0, ROWS, put, 0)
        return carry

    lax.fori_loop(0, 2, second, 0)
    halo_send(0)
    sum_middle(0)
    products(1, 0, False)

    def advance(alpha, beta, slot):
        def body(r, carry):
            for part in range(3):
                for t in range(2):
                    at = (part, r, pl.ds(8 * t, 8), slice(None))
                    v, tt, w, y = v_out[at], total[at], rate[at], own(slot, part, r, t)
                    v = alpha * v + beta * tt
                    w = alpha * w + beta * y
                    v_out[at] = v
                    u_out[at] = u_out[at] + v
                    rate[at] = w
                    total[at] = tt + w
            return carry

        lax.fori_loop(0, ROWS, body, 0)

    def cycle(n, carry):
        alpha, beta = carry
        slot = lax.rem(n, 2)
        other = 1 - slot
        local_pass(slot, field, bond, diag, force)
        sum_middle(n + 1)
        halo_wait(slot)
        across_pass(slot, near, far, bond, force)
        along_pass(slot, rim, bond_edge, force)
        alpha, beta = damping_of(n, alpha, beta)

        def body(r, carry):
            for part in range(3):
                for t in range(2):
                    at = (part, r, pl.ds(8 * t, 8), slice(None))
                    x = alpha * pull[at] + beta * force[at]
                    pull[at] = x
                    field[other, part, 3 + r, pl.ds(PAD + 8 * t, 8), :] = own(slot, part, r, t) + x
            return carry

        lax.fori_loop(0, ROWS, body, 0)

        @pl.when(n < ITERS - 3)
        def _():
            halo_send(other)

        advance(alpha, beta, slot)
        products(n + 2, other, False)
        return alpha, beta

    one = jnp.ones((8, DEPTH), F32)
    alpha, beta = lax.fori_loop(0, ITERS - 2, cycle, (one, jnp.zeros((8, DEPTH), F32)))
    sum_middle(ITERS - 1)
    alpha, beta = damping_of(ITERS - 2, alpha, beta)
    advance(alpha, beta, (ITERS - 2) % 2)
    alpha, beta = damping_of(ITERS - 1, alpha, beta)

    def finish(r, carry):
        for part in range(3):
            for t in range(2):
                at = (part, r, pl.ds(8 * t, 8), slice(None))
                v = alpha * v_out[at] + beta * total[at]
                v_out[at] = v
                u_out[at] = u_out[at] + v
        return carry

    lax.fori_loop(0, ROWS, finish, 0)


def on_device(nx, ny, disp, vel, load, flags, mask_bits):
    block = (3, ROWS, COLS, DEPTH)
    any_spec = pl.BlockSpec(memory_space=pl.ANY)
    vmem_spec = pl.BlockSpec(memory_space=pltpu.VMEM)
    turns = ITERS
    dma = pltpu.SemaphoreType.DMA
    scratch = [
        pltpu.VMEM((SLOTS, 3, TALL, WIDE, DEPTH), F32),
        pltpu.VMEM((SLOTS, 2, 3, 2, WIDE, DEPTH), F32),
        pltpu.VMEM((SLOTS, 2, WIDE, DEPTH), F32),
        pltpu.VMEM((SLOTS, 2, 7, 24, DEPTH), F32),
        pltpu.VMEM((SLOTS, 4, 16, DEPTH), F32),
        pltpu.VMEM((SLOTS, 2, 7, 8, DEPTH), F32),
        pltpu.VMEM((SLOTS, 4, 16, DEPTH), F32),
        pltpu.VMEM((4, TALL, WIDE, DEPTH), I32),
        pltpu.VMEM((2, 4, 3, 8, DEPTH), I32),
        pltpu.VMEM((4, 16, DEPTH), I32),
        pltpu.VMEM((2, 4, 3, 8, DEPTH), I32),
        pltpu.VMEM((4, 16, DEPTH), I32),
        pltpu.VMEM((BONDS, ROWS * COLS, DEPTH), F32),
        pltpu.VMEM((2, len(EDGE), ROWS, DEPTH), F32),
        pltpu.VMEM((6, ROWS, COLS, DEPTH), F32),
        pltpu.VMEM(block, F32),
        pltpu.VMEM((2,) + block, F32),
        pltpu.VMEM((2,) + block, F32),
        pltpu.VMEM(block, F32),
        pltpu.VMEM(block[1:], I32),
        pltpu.VMEM((turns, nx, 8, DEPTH), F32),
        pltpu.VMEM((turns, ny, 8, DEPTH), F32),
        dma((7,)),
        dma((SLOTS, 10)),
        dma((SLOTS, 10)),
        dma((8,)),
        dma((8,)),
        dma((2, turns)),
        dma((2, turns)),
    ]
    return pl.pallas_call(
        functools.partial(kernel, nx, ny),
        out_shape=[jax.ShapeDtypeStruct(block, F32)] * 2,
        in_specs=[any_spec] * 5,
        out_specs=[vmem_spec] * 2,
        scratch_shapes=scratch,
        compiler_params=pltpu.CompilerParams(
            collective_id=0, has_side_effects=True, vmem_limit_bytes=40 * 1024 * 1024
        ),
    )(disp, vel, load, flags, mask_bits)


def solution(mesh):
    split = P(None, "gx", "gy", None)
    return jax.shard_map(
        functools.partial(on_device, mesh.shape["gx"], mesh.shape["gy"]),
        mesh=mesh,
        in_specs=(split, split, split, P("gx", "gy", None), split),
        out_specs=(split, split),
        check_vma=False,
    )
```

```python
import functools
import math

import jax
import jax.numpy as jnp
from jax import lax
from jax.experimental import pallas as pl
from jax.experimental.pallas import tpu as pltpu
from jax.sharding import PartitionSpec as P

ITERS = 8
MASS = 64.0
EPSILON = 1e-06
ROWS = 8
COLS = 16
DEPTH = 128
PAD = 8
WIDE = COLS + 2 * PAD
TALL = ROWS + 6
GROUP = 4
SLOTS = 4
F32 = jnp.float32
I32 = jnp.int32


def neighbour_table():
    table = []
    for across in range(-3, 4):
        for along in range(-3, 4):
            for upward in range(-3, 4):
                length = across * across + along * along + upward * upward
                if 0 < length <= 9:
                    table.append((across, along, upward))
    return table


TABLE = neighbour_table()
NUMBER = {offset: k for k, offset in enumerate(TABLE)}
BONDS = len(TABLE)


def on_axis(offset):
    return sum(1 for part in offset if part) == 1


def weight_of(offset):
    length = float(sum(part * part for part in offset))
    weight = 1.0 / (length * math.sqrt(length))
    return weight * length if on_axis(offset) else weight


def oblique(b, c):
    return [a for a in range(-2, 3) if (a, b, c) in NUMBER and not on_axis((a, b, c))]


EDGE = []
for _c in range(-2, 3):
    for _reach in (1, 2, 3):
        for _a in range(-2, 3):
            if (_a, _reach, _c) in NUMBER:
                for _j in range(_reach):
                    EDGE.append((_a, _reach, _c, _j, _reach - 1 - _j))
EDGE_AT = {entry[:4]: n for n, entry in enumerate(EDGE)}


def add(total, term):
    return term if total is None else total + term


def sub(total, term):
    return -term if total is None else total - term


def scaled(factor, value):
    if factor == 1:
        return value
    if factor == -1:
        return -value
    return float(factor) * value


def plus_scaled(total, factor, value):
    if total is None:
        return scaled(factor, value)
    if factor == 1:
        return total + value
    if factor == -1:
        return total - value
    return total + float(factor) * value


def combine(weights, totals):
    out = None
    for factor, value in zip(weights, totals):
        if factor and value is not None:
            out = plus_scaled(out, factor, value)
    return out


def accumulate_first(total, factor, value):
    if factor == 0 or value is None:
        return total
    if factor == 2:
        return value
    if factor == -2:
        return 2.0 * (total - value)
    return plus_scaled(total, factor, value)


def turned(value, c):
    if c == 0:
        return value
    return pltpu.roll(value, (-c) % DEPTH, 1)


def moments(terms):
    zeroth = None
    for a in sorted(terms):
        zeroth = add(zeroth, terms[a])
    first = None
    if 2 in terms:
        first = add(first, terms[2])
    if -2 in terms:
        first = sub(first, terms[-2])
    if first is not None:
        first = 2.0 * first
    if 1 in terms:
        first = add(first, terms[1])
    if -1 in terms:
        first = sub(first, terms[-1])
    return zeroth, first


def local_pass(slot, field, bond, diag, out):
    def group(g, carry):
        base = g * GROUP
        for t in range(2):
            col = PAD + 8 * t

            def coef(offset, i):
                start = pl.multiple_of((base + i) * COLS + 8 * t, 8)
                return bond[NUMBER[offset], pl.ds(start, 8), :]

            def source(part, i, b):
                return field[slot, part, base + 3 + i, pl.ds(col + b, 8), :]

            for c in (0, 1, -1, 2, -2, 3, -3):
                g0 = [None] * GROUP
                g1 = [None] * GROUP
                g2 = [None] * GROUP
                if c:
                    for i in range(GROUP):
                        g2[i] = coef((0, 0, c), i) * source(2, i, 0)
                if c == 0:
                    for i in range(GROUP):
                        for a in (1, -1, 2, -2, 3, -3):
                            g0[i] = add(g0[i], coef((a, 0, 0), i) * source(0, i + a, 0))
                        for b in (1, -1, 2, -2, 3, -3):
                            g1[i] = add(g1[i], coef((0, b, 0), i) * source(1, i, b))
                if abs(c) < 3:
                    n0 = [None] * GROUP
                    n1 = [None] * GROUP
                    for b in (2, -2, 1, -1, 0):
                        reach = oblique(b, c)
                        if not reach:
                            continue
                        span = range(min(reach), GROUP + max(reach))
                        u0 = {i: source(0, i, b) for i in span}
                        twice = {i: 2.0 * u0[i] for i in span} if 2 in reach else None
                        u1 = {i: source(1, i, b) if b else None for i in span}
                        u2 = {i: source(2, i, b) if c else None for i in span}
                        s = {i: combine((b, c), (u1[i], u2[i])) for i in span}
                        for i in range(GROUP):
                            terms = {}
                            for a in reach:
                                near = s[i + a]
                                if abs(a) == 1:
                                    near = near + u0[i + a] if a > 0 else near - u0[i + a]
                                elif a:
                                    near = near + twice[i + a] if a > 0 else near - twice[i + a]
                                terms[a] = coef((a, b, c), i) * near
                            zeroth, first = moments(terms)
                            g0[i] = add(g0[i], first)
                            if c:
                                n0[i] = add(n0[i], zeroth)
                            if b == 2:
                                n1[i] = zeroth
                            elif b == -2:
                                n1[i] = 2.0 * (n1[i] - zeroth)
                            elif b:
                                n1[i] = plus_scaled(n1[i], b, zeroth)
                    for i in range(GROUP):
                        g1[i] = add(g1[i], n1[i])
                        if c:
                            g2[i] = plus_scaled(g2[i], c, n0[i])
                for i in range(GROUP):
                    for part, value in enumerate((g0[i], g1[i], g2[i])):
                        if c == 0:
                            if diag is not None:
                                u = [source(other, i, 0) for other in range(3)]
                                value = less_diagonal(value, diag, part, base + i, t, u)
                            elif value is None:
                                value = jnp.zeros((8, DEPTH), F32)
                            out[part, base + i, pl.ds(8 * t, 8), :] = value
                        elif value is not None:
                            out[part, base + i, pl.ds(8 * t, 8), :] += turned(value, c)
        return carry

    lax.fori_loop(0, ROWS // GROUP, group, 0)


def less_diagonal(value, diag, part, r, t, u):
    own = None
    for other in range(3):
        pair = DIAG[min(part, other), max(part, other)]
        own = add(own, diag[pair, r, pl.ds(8 * t, 8), :] * u[other])
    return -own if value is None else value - own


DIAG = {(0, 0): 0, (0, 1): 1, (1, 1): 2, (0, 2): 3, (1, 2): 4, (2, 2): 5}


def across_pass(slot, near, far, bond, out):
    for side in range(2):
        sign = 1 if side else -1
        edge = ROWS - 1 if side else 0
        for t in range(2):
            col = PAD + 8 * t

            def coef(offset, i):
                return bond[NUMBER[offset], pl.ds((edge - sign * i) * COLS + 8 * t, 8), :]

            def source(part, layer, b):
                e = layer if side else 1 - layer
                return near[slot, side, part, e, pl.ds(col + b, 8), :]

            sums = [[None] * 3 for i in range(2)]
            third = None
            for c in (0, 1, -1, 2, -2):
                g = [[None] * 3 for i in range(2)]
                if c == 0:
                    for layer in range(2):
                        u0 = source(0, layer, 0)
                        for i in range(3):
                            a = sign * (i + layer + 1)
                            if abs(a) <= 3:
                                term = coef((a, 0, 0), i) * u0
                                if i < 2:
                                    g[i][0] = add(g[i][0], term)
                                else:
                                    third = term
                    g[0][0] = g[0][0] + coef((3 * sign, 0, 0), 0) * far[slot, side, pl.ds(col, 8), :]
                n0 = [None] * 2
                n1 = [None] * 2
                deep = [None] * 2
                for b in (2, -2, 1, -1, 0):
                    reach = oblique(b, c)
                    if not reach:
                        continue
                    zeroth = [None] * 2
                    for layer in range(max(reach)):
                        u0 = source(0, layer, b)
                        u1 = source(1, layer, b) if b else None
                        u2 = source(2, layer, b) if c else None
                        s = combine((b, c), (u1, u2))
                        for i in range(2):
                            size = i + layer + 1
                            a = sign * size
                            if a not in reach:
                                continue
                            if size == 2 and i == 1:
                                q = plus_scaled(q, sign, u0)
                            else:
                                q = plus_scaled(s, a, u0)
                            term = coef((a, b, c), i) * q
                            zeroth[i] = add(zeroth[i], term)
                            if size == 1:
                                g[i][0] = plus_scaled(g[i][0], sign, term)
                            else:
                                deep[i] = add(deep[i], term)
                    for i in range(2):
                        if zeroth[i] is None:
                            continue
                        if c:
                            n0[i] = add(n0[i], zeroth[i])
                        n1[i] = accumulate_first(n1[i], b, zeroth[i])
                for i in range(2):
                    if deep[i] is not None:
                        g[i][0] = plus_scaled(g[i][0], 2 * sign, deep[i])
                for i in range(2):
                    g[i][1] = n1[i]
                    g[i][2] = scaled(c, n0[i]) if c else None
                    for part in range(3):
                        if g[i][part] is not None:
                            sums[i][part] = add(sums[i][part], turned(g[i][part], c))
            for i in range(2):
                row = edge - sign * i
                for part in range(3):
                    out[part, row, pl.ds(8 * t, 8), :] += sums[i][part]
            out[0, edge - 2 * sign, pl.ds(8 * t, 8), :] += third


def along_terms(slot, rim, bond_edge):
    found = []
    for side in range(2):
        sign = 1 if side else -1

        def coef(a, size, c, j):
            return bond_edge[side, EDGE_AT[a, size, c, j]]

        def source(part, layer, a):
            return rim[slot, side, part * 2 + layer, pl.ds(8 + a, 8), :]

        sums = [[None] * 3 for j in range(2)]
        third = None
        for c in (0, 1, -1, 2, -2):
            g = [[None] * 3 for j in range(2)]
            if c == 0:
                for layer in range(3):
                    at = 6 if layer == 2 else 2 + layer
                    u1 = rim[slot, side, at, pl.ds(8, 8), :]
                    for j in range(3 - layer):
                        term = coef(0, layer + 1 + j, 0, j) * u1
                        if j < 2:
                            g[j][1] = add(g[j][1], term)
                        else:
                            third = term
            n0 = [None] * 2
            n1 = [None] * 2
            deep = [None] * 2
            for a in (2, -2, 1, -1, 0):
                reach = [size for size in (1, 2) if (a, size, c) in NUMBER and not on_axis((a, size, c))]
                if not reach:
                    continue
                zeroth = [None] * 2
                for layer in range(max(reach)):
                    u0 = source(0, layer, a) if a else None
                    u1 = source(1, layer, a)
                    u2 = source(2, layer, a) if c else None
                    s = combine((a, c), (u0, u2))
                    for j in range(2):
                        size = j + layer + 1
                        if size not in reach:
                            continue
                        if size == 2 and j == 1:
                            q = plus_scaled(q, sign, u1)
                        else:
                            q = plus_scaled(s, sign * size, u1)
                        term = coef(a, size, c, j) * q
                        zeroth[j] = add(zeroth[j], term)
                        if size == 1:
                            g[j][1] = plus_scaled(g[j][1], sign, term)
                        else:
                            deep[j] = add(deep[j], term)
                for j in range(2):
                    if zeroth[j] is None:
                        continue
                    if c:
                        n0[j] = add(n0[j], zeroth[j])
                    n1[j] = accumulate_first(n1[j], a, zeroth[j])
            for j in range(2):
                if deep[j] is not None:
                    g[j][1] = plus_scaled(g[j][1], 2 * sign, deep[j])
            for j in range(2):
                g[j][0] = n1[j]
                g[j][2] = scaled(c, n0[j]) if c else None
                for part in range(3):
                    if g[j][part] is not None:
                        sums[j][part] = add(sums[j][part], turned(g[j][part], c))
        found.append([(part, j, sums[j][part]) for part in range(3) for j in range(2)] + [(1, 2, third)])
    return found


def spread(found, put):
    for side in range(2):
        for part, j, value in found[side]:
            at = COLS - 1 - j if side else j
            for r in range(ROWS):
                put(part, r, at, value[r : r + 1, :])


def weight_if_intact(near, far, offset):
    k = NUMBER[offset]
    word, bit = divmod(k, 31)
    far_word, far_bit = divmod(BONDS - 1 - k, 31)
    broken = (near[word] & I32(1 << bit)) | (far(far_word) & I32(1 << far_bit))
    return jnp.where(broken == 0, F32(weight_of(offset)), F32(0.0))


def moved(own, c):
    if not c:
        return own
    lane = lax.broadcasted_iota(I32, (8, DEPTH), 1)
    outside = lane < c if c > 0 else lane >= DEPTH + c
    return [jnp.where(outside, I32(-1), pltpu.roll(word, c % DEPTH, 1)) for word in own]


def tally(sums, offset, value):
    a, b, c = offset
    if on_axis(offset):
        at = 0 if a else (2 if b else 5)
        sums[at] = add(sums[at], value)
        return
    for at, factor in enumerate((a * a, a * b, b * b, a * c, b * c, c * c)):
        if factor:
            sums[at] = plus_scaled(sums[at], factor, value)


def build_bonds(words, bond, diag):
    def row(r, carry):
        for t in range(2):
            start = pl.multiple_of(r * COLS + 8 * t, 8)
            own = [words[w, r + 3, pl.ds(PAD + 8 * t, 8), :] for w in range(4)]
            totals = [None] * 6
            for c in range(-3, 4):
                near = moved(own, c)
                sums = [None] * 6
                for b in range(-3, 4):
                    values = {}
                    for a in range(-3, 4):
                        k = NUMBER.get((a, b, c))
                        if k is None:
                            continue

                        def far(w):
                            return words[w, r + 3 + a, pl.ds(PAD + 8 * t + b, 8), :]

                        value = weight_if_intact(near, far, (a, b, c))
                        bond[k, pl.ds(start, 8), :] = value
                        if on_axis((a, b, c)):
                            tally(sums, (a, b, c), value)
                        else:
                            values[a] = value
                    if not values:
                        continue
                    zeroth, first = moments(values)
                    second = None
                    if 2 in values:
                        second = 4.0 * (values[2] + values[-2])
                    second = add(second, values[1] + values[-1])
                    sums[0] = add(sums[0], second)
                    if b:
                        sums[1] = plus_scaled(sums[1], b, first)
                        sums[2] = plus_scaled(sums[2], b * b, zeroth)
                    if c:
                        sums[3] = plus_scaled(sums[3], c, first)
                        sums[5] = plus_scaled(sums[5], c * c, zeroth)
                        if b:
                            sums[4] = plus_scaled(sums[4], b * c, zeroth)
                for n in range(6):
                    if sums[n] is not None:
                        totals[n] = add(totals[n], turned(sums[n], c))
            for n in range(6):
                diag[n, r, pl.ds(8 * t, 8), :] = totals[n]
        return carry

    lax.fori_loop(0, ROWS, row, 0)


def build_across(words, words_near, bond, diag):
    for side in range(2):
        sign = 1 if side else -1
        edge = ROWS - 1 if side else 0
        for t in range(2):
            for i in range(3):
                r = edge - sign * i
                own = [words[w, r + 3, pl.ds(PAD + 8 * t, 8), :] for w in range(4)]
                totals = [None] * 6
                for c in range(-2, 3):
                    if i == 2 and c:
                        continue
                    near = moved(own, c)
                    sums = [None] * 6
                    for b in range(-2, 3):
                        for layer in range(3 - i):
                            offset = (sign * (i + layer + 1), b, c)
                            if offset not in NUMBER:
                                continue

                            def far(w):
                                e = layer if side else 2 - layer
                                return words_near[side, w, e, pl.ds(PAD + 8 * t + b, 8), :]

                            value = weight_if_intact(near, far, offset)
                            bond[NUMBER[offset], pl.ds(r * COLS + 8 * t, 8), :] = value
                            tally(sums, offset, value)
                    for n in range(6):
                        if sums[n] is not None:
                            totals[n] = add(totals[n], turned(sums[n], c))
                for n in range(6):
                    if totals[n] is not None:
                        diag[n, r, pl.ds(8 * t, 8), :] += totals[n]


def build_along(words_mine, words_rim, bond_edge, diag):
    for side in range(2):
        sign = 1 if side else -1
        edge = COLS - 1 if side else 0
        for j in range(3):
            own = [words_mine[1 - side, w, j] for w in range(4)]
            totals = [None] * 6
            for c in range(-2, 3):
                if j == 2 and c:
                    continue
                near = moved(own, c)
                sums = [None] * 6
                for n, (a, size, up, col, layer) in enumerate(EDGE):
                    if col != j or up != c:
                        continue
                    offset = (a, sign * size, c)

                    def far(w):
                        return words_rim[side, w, layer, pl.ds(8 + a, 8), :]

                    value = weight_if_intact(near, far, offset)
                    bond_edge[side, n] = value
                    tally(sums, offset, value)
                for n in range(6):
                    if sums[n] is not None:
                        totals[n] = add(totals[n], turned(sums[n], c))
            at = edge - sign * j
            for n in range(6):
                if totals[n] is not None:
                    for r in range(ROWS):
                        diag[n, r, at : at + 1, :] += totals[n][r : r + 1, :]


def kernel(
    nx, ny,
    disp, vel, load, flags, mask,
    u_out, v_out,
    field, near, far, rim, corner, rim_send, corner_send,
    words, words_near, words_rim, words_corner, words_rim_send, words_corner_send,
    bond, bond_edge, diag,
    pool, load_buf, flag_buf,
    ring_one, ring_two,
    in_sem, send_sem, recv_sem, word_send, word_recv, sum_send, sum_recv,
):
    total, rate, force, pull = (pool.at[n] for n in range(4))
    ax = lax.axis_index("gx")
    ay = lax.axis_index("gy")
    here = {-1: (ax > 0, ay > 0), 1: (ax < nx - 1, ay < ny - 1)}

    def exists(dx, dy):
        cond = None
        if dx:
            cond = here[dx][0]
        if dy:
            other = here[dy][1]
            cond = other if cond is None else cond & other
        return cond

    def device(dx, dy):
        return {"gx": ax + dx, "gy": ay + dy}

    sides = [(dx, dy) for dx in (-1, 0, 1) for dy in (-1, 0, 1) if dx or dy]
    diagonals = [(dx, dy) for dx, dy in sides if dx and dy]

    own_rows = pl.ds(3, ROWS)
    own_cols = pl.ds(PAD, COLS)
    loads = [
        pltpu.make_async_copy(mask, words.at[:, own_rows, own_cols], in_sem.at[0]),
        pltpu.make_async_copy(vel, field.at[1, :, own_rows, own_cols], in_sem.at[1]),
        pltpu.make_async_copy(disp, field.at[0, :, own_rows, own_cols], in_sem.at[2]),
        pltpu.make_async_copy(disp, u_out, in_sem.at[3]),
        pltpu.make_async_copy(vel, v_out, in_sem.at[4]),
        pltpu.make_async_copy(load, load_buf, in_sem.at[5]),
        pltpu.make_async_copy(flags, flag_buf, in_sem.at[6]),
    ]
    for copy in loads:
        copy.start()

    zero8 = jnp.zeros((8, DEPTH), F32)

    barrier = pltpu.get_barrier_semaphore()
    for step in range(1, nx):
        pl.semaphore_signal(barrier, inc=1, device_id={"gx": lax.rem(ax + step, nx), "gy": ay})
    for step in range(1, ny):
        pl.semaphore_signal(barrier, inc=1, device_id={"gx": ax, "gy": lax.rem(ay + step, ny)})
    for dx, dy in diagonals:
        where = {"gx": lax.rem(ax + dx + nx, nx), "gy": lax.rem(ay + dy + ny, ny)}
        pl.semaphore_signal(barrier, inc=1, device_id=where)


    inner = slice(PAD, PAD + COLS)
    pads = (slice(0, PAD), slice(PAD + COLS, WIDE))
    borders = list(range(3)) + list(range(TALL - 3, TALL))

    def broken(*shape):
        return jnp.full(shape + (DEPTH,), -1, I32)

    def clear():
        def slot_clear(slot, carry):
            for part in range(3):
                for r in borders:
                    field[slot, part, r] = jnp.zeros((WIDE, DEPTH), F32)
                for r in range(3, TALL - 3):
                    for pad in pads:
                        field[slot, part, r, pad, :] = zero8
                for side in range(2):
                    for e in range(2):
                        for pad in pads:
                            near[slot, side, part, e, pad, :] = zero8
            for side in range(2):
                for at in range(7):
                    rim[slot, side, at, 0:8, :] = zero8
                    rim[slot, side, at, 16:24, :] = zero8
            return carry

        lax.fori_loop(0, SLOTS, slot_clear, 0)
        for w in range(4):
            for r in range(TALL):
                if r in borders:
                    words[w, r] = broken(WIDE)
                else:
                    for pad in pads:
                        words[w, r, pad, :] = broken(PAD)
            for side in range(2):
                for layer in range(3):
                    for pad in pads:
                        words_near[side, w, layer, pad, :] = broken(PAD)
                    words_rim[side, w, layer, 0:8, :] = broken(8)
                    words_rim[side, w, layer, 16:24, :] = broken(8)
        for side in range(2):
            @pl.when(ax == (nx - 1 if side else 0))
            def _():
                for slot in range(SLOTS):
                    far[slot, side, inner, :] = jnp.zeros((COLS, DEPTH), F32)
                    for part in range(3):
                        for e in range(2):
                            near[slot, side, part, e, inner, :] = jnp.zeros((COLS, DEPTH), F32)
                for w in range(4):
                    for layer in range(3):
                        words_near[side, w, layer, inner, :] = broken(COLS)

            @pl.when(ay == (ny - 1 if side else 0))
            def _():
                for slot in range(SLOTS):
                    for at in range(7):
                        rim[slot, side, at, 8:16, :] = zero8
                for w in range(4):
                    for layer in range(3):
                        words_rim[side, w, layer, 8:16, :] = broken(8)

    def edge_rows(dx):
        return (0, 2) if dx < 0 else (ROWS - 2, ROWS - 3)

    def halo_copies(slot, dx, dy):
        into = {-1: 1, 1: 0}
        if dx and dy:
            n = into[dx] * 2 + into[dy]
            return [(corner_send.at[slot, n], corner.at[slot, n], 6 + n)]
        if dx:
            first, third = edge_rows(dx)
            side = into[dx]
            return [
                (
                    field.at[slot, :, pl.ds(3 + first, 2), own_cols],
                    near.at[slot, side, :, :, own_cols],
                    side,
                ),
                (field.at[slot, 0, 3 + third, own_cols], far.at[slot, side, own_cols], 2 + side),
            ]
        side = into[dy]
        return [(rim_send.at[slot, side], rim.at[slot, side, :, pl.ds(8, 8)], 4 + side)]

    def spot(part, layer):
        return 6 if layer == 2 else part * 2 + layer

    def pack_rim(slot):
        for side in range(2):
            for part in range(3):
                for layer in range(3 if part == 1 else 2):
                    col = PAD + (layer if side else COLS - 1 - layer)
                    for r in range(ROWS):
                        rim_send[slot, side, spot(part, layer), r : r + 1, :] = field[
                            slot, part, 3 + r, col : col + 1, :
                        ]

    def ends(dx):
        return slice(0, 2) if dx < 0 else slice(ROWS - 2, ROWS)

    def beyond(dx):
        return slice(6, 8) if dx < 0 else slice(16, 18)

    def copy_of(slot, dx, dy, src, dst, n):
        return pltpu.make_async_remote_copy(
            src_ref=src, dst_ref=dst, send_sem=send_sem.at[slot, n], recv_sem=recv_sem.at[slot, n],
            device_id=device(dx, dy),
        )

    along = [(0, -1), (0, 1)]
    across = [(-1, 0), (1, 0)]

    def send_all(slot, which):
        for dx, dy in which:
            @pl.when(exists(dx, dy))
            def _():
                for src, dst, n in halo_copies(slot, dx, dy):
                    copy_of(slot, dx, dy, src, dst, n).start()

    def send_rim(slot):
        send_all(slot, along)
        for dx, dy in diagonals:
            n = (1 if dx < 0 else 0) * 2 + (1 if dy < 0 else 0)
            for at in range(6):
                corner_send[slot, n, 2 * at : 2 * at + 2, :] = rim_send[slot, 1 if dy < 0 else 0, at, ends(dx), :]
        send_all(slot, diagonals)

    def halo_send(slot):
        pack_rim(slot)
        send_rim(slot)
        send_all(slot, across)

    def wait_all(slot, which):
        for dx, dy in which:
            @pl.when(exists(dx, dy))
            def _():
                for src, dst, n in halo_copies(slot, dx, dy):
                    copy_of(slot, dx, dy, src, dst, n).wait_send()
                for src, dst, n in halo_copies(slot, -dx, -dy):
                    copy_of(slot, dx, dy, src, dst, n).wait_recv()

    def wait_rim(slot):
        wait_all(slot, along + diagonals)
        for dx, dy in diagonals:
            sx, sy = (1 if dx > 0 else 0), (1 if dy > 0 else 0)

            @pl.when(exists(dx, dy))
            def _():
                for at in range(6):
                    rim[slot, sy, at, beyond(dx), :] = corner[slot, sx * 2 + sy, 2 * at : 2 * at + 2, :]

    def word_copies(dx, dy):
        into = {-1: 1, 1: 0}
        if dx and dy:
            n = into[dx] * 2 + into[dy]
            return [(words_corner_send.at[n], words_corner.at[n], 4 + n)]
        if dx:
            first = 3 if dx < 0 else ROWS
            return [(words.at[:, pl.ds(first, 3), own_cols], words_near.at[into[dx], :, :, own_cols], into[dx])]
        side = into[dy]
        return [(words_rim_send.at[side], words_rim.at[side, :, :, pl.ds(8, 8)], 2 + side)]

    def word_copy(dx, dy, src, dst, n):
        return pltpu.make_async_remote_copy(
            src_ref=src, dst_ref=dst, send_sem=word_send.at[n], recv_sem=word_recv.at[n], device_id=device(dx, dy),
        )

    loads[0].wait()
    for side in range(2):
        for w in range(4):
            for layer in range(3):
                col = PAD + (layer if side else COLS - 1 - layer)
                for r in range(ROWS):
                    words_rim_send[side, w, layer, r : r + 1, :] = words[w, 3 + r, col : col + 1, :]
    for dx, dy in diagonals:
        n = (1 if dx < 0 else 0) * 2 + (1 if dy < 0 else 0)
        for w in range(4):
            for layer in range(2):
                at = (w * 2 + layer) * 2
                words_corner_send[n, at : at + 2, :] = words_rim_send[1 if dy < 0 else 0, w, layer, ends(dx), :]
    pl.semaphore_wait(barrier, nx + ny + 2)
    for dx, dy in sides:
        @pl.when(exists(dx, dy))
        def _():
            for src, dst, n in word_copies(dx, dy):
                word_copy(dx, dy, src, dst, n).start()
    for n in range(2):
        loads[2 - n].wait()
        halo_send(n)

    clear()
    build_bonds(words, bond, diag)
    def words_wait():
        for dx, dy in sides:
            @pl.when(exists(dx, dy))
            def _():
                for src, dst, n in word_copies(dx, dy):
                    word_copy(dx, dy, src, dst, n).wait_send()
                for src, dst, n in word_copies(-dx, -dy):
                    word_copy(dx, dy, src, dst, n).wait_recv()
        for dx, dy in diagonals:
            sx, sy = (1 if dx > 0 else 0), (1 if dy > 0 else 0)

            @pl.when(exists(dx, dy))
            def _():
                for w in range(4):
                    for layer in range(2):
                        at = (w * 2 + layer) * 2
                        words_rim[sy, w, layer, beyond(dx), :] = words_corner[sx * 2 + sy, at : at + 2, :]

        build_across(words, words_near, bond, diag)
        build_along(words_rim_send, words_rim, bond_edge, diag)

    def sum_copy(src, dst, which, turn, where):
        return pltpu.make_async_remote_copy(
            src_ref=src, dst_ref=dst, send_sem=sum_send.at[which, turn], recv_sem=sum_recv.at[which, turn],
            device_id=where,
        )

    def sum_begin(turn, rows):
        slab = jnp.concatenate([jnp.sum(row, axis=0, keepdims=True) for row in rows] + [jnp.zeros((2, DEPTH), F32)], axis=0)
        each = jnp.broadcast_to(jnp.sum(slab, axis=1, keepdims=True), (8, DEPTH))
        mine = lax.broadcasted_iota(I32, (8, DEPTH), 0) == lax.broadcasted_iota(I32, (8, DEPTH), 1)
        ring_one[turn, ax] = jnp.sum(jnp.where(mine, each, 0.0), axis=0, keepdims=True)
        for step in range(1, nx):
            sum_copy(
                ring_one.at[turn, ax], ring_one.at[turn, ax], 0, turn, {"gx": lax.rem(ax + step, nx), "gy": ay}
            ).start()

    def sum_middle(turn):
        some = ring_one.at[turn, pl.ds(0, nx - 1)]
        copy = sum_copy(some, some, 0, turn, {"gx": ax, "gy": ay})
        copy.wait_recv()
        copy.wait_send()
        ring_two[turn, ay] = jnp.sum(ring_one[turn], axis=0)
        for step in range(1, ny):
            sum_copy(
                ring_two.at[turn, ay], ring_two.at[turn, ay], 1, turn, {"gx": ax, "gy": lax.rem(ay + step, ny)}
            ).start()

    def sum_end(turn):
        some = ring_two.at[turn, pl.ds(0, ny - 1)]
        copy = sum_copy(some, some, 1, turn, {"gx": ax, "gy": ay})
        copy.wait_recv()
        copy.wait_send()
        row = jnp.sum(ring_two[turn], axis=0)
        return [jnp.broadcast_to(row[:, n : n + 1], (8, DEPTH)) for n in range(6)]

    count = 3.0 * ROWS * nx * COLS * ny * DEPTH

    def damping_of(turn, alpha, beta):
        g0, g1, g2, h0, h1, h2 = sum_end(turn)
        kinetic = alpha * alpha * g0 + 2.0 * alpha * beta * g1 + beta * beta * g2
        rayleigh = -(alpha * alpha * h0 + alpha * beta * h1 + beta * beta * h2)
        rayleigh = jnp.maximum(rayleigh, 0.0)
        damping = 2.0 * jnp.sqrt((rayleigh / count) / (MASS * (kinetic / count + EPSILON)))
        return (2.0 - damping) / (2.0 + damping), 2.0 / (MASS * (2.0 + damping))

    def own(ref_slot, part, r, t):
        return field[ref_slot, part, 3 + r, pl.ds(PAD + 8 * t, 8), :]

    vregs = [(part, r, t) for part in range(3) for r in range(ROWS) for t in range(2)]

    def products(turn, slot, first):
        def body(r, carry):
            acc = list(carry)
            for part in range(3):
                for t in range(2):
                    at = (part, r, pl.ds(8 * t, 8), slice(None))
                    v, w = v_out[at], rate[at]
                    acc[0] += v * v
                    acc[3] += v * w
                    if not first:
                        tt, y = total[at], own(slot, part, r, t)
                        acc[1] += v * tt
                        acc[2] += tt * tt
                        acc[4] += v * y + tt * w
                        acc[5] += tt * y
            return tuple(acc)

        sum_begin(turn, lax.fori_loop(0, ROWS, body, (zero8,) * 6))

    def rest(slot, out):
        wait_all(slot, across)
        across_pass(slot, near, far, bond, out)
        wait_rim(slot)

        def put(part, r, at, value):
            out[part, r, at : at + 1, :] += value

        spread(along_terms(slot, rim, bond_edge), put)

    for copy in loads[3:]:
        copy.wait()

    def begin(n, carry):
        out = pool.at[n]
        local_pass(n, field, bond, None, out)

        @pl.when(n == 0)
        def _():
            words_wait()

        rest(n, out)
        loaded = lax.div(3 - n, 3).astype(F32)
        to = lax.rem(n + 2, 4)

        def put(r, carry):
            for t in range(2):
                at = (r, pl.ds(8 * t, 8), slice(None))
                active = loaded * flag_buf[at].astype(F32)
                u = [own(n, part, r, t) for part in range(3)]
                for part in range(3):
                    value = less_diagonal(out[(part,) + at], diag, part, r, t, u)
                    value = value + active * load_buf[(part,) + at]
                    out[(part,) + at] = value
                    field[to, part, 3 + r, pl.ds(PAD + 8 * t, 8), :] = value
            return carry

        lax.fori_loop(0, ROWS, put, 0)

        @pl.when(n < 3)
        def _():
            halo_send(to)

        @pl.when(n == 1)
        def _():
            products(0, 0, True)

        @pl.when(n == 2)
        def _():
            sum_middle(0)
            products(1, 0, False)

        return carry

    lax.fori_loop(0, 4, begin, 0)

    def advance(alpha, beta, slot):
        def body(r, carry):
            for part in range(3):
                for t in range(2):
                    at = (part, r, pl.ds(8 * t, 8), slice(None))
                    v, tt, w, y = v_out[at], total[at], rate[at], own(slot, part, r, t)
                    v = alpha * v + beta * tt
                    w = alpha * w + beta * y
                    v_out[at] = v
                    u_out[at] = u_out[at] + v
                    rate[at] = w
                    total[at] = tt + w
            return carry

        lax.fori_loop(0, ROWS, body, 0)

    def cycle(n, carry):
        alpha, beta = carry
        slot = lax.rem(n, 2)
        other = 1 - slot
        local_pass(slot, field, bond, diag, force)
        wait_all(slot, across)
        across_pass(slot, near, far, bond, force)
        sum_middle(n + 1)
        alpha, beta = damping_of(n, alpha, beta)

        def body(r, carry):
            for part in range(3):
                for t in range(2):
                    at = (part, r, pl.ds(8 * t, 8), slice(None))
                    x = alpha * pull[at] + beta * force[at]
                    pull[at] = x
                    field[other, part, 3 + r, pl.ds(PAD + 8 * t, 8), :] = own(slot, part, r, t) + x
            return carry

        lax.fori_loop(0, ROWS, body, 0)
        pack_rim(other)
        wait_rim(slot)
        terms = [[(part, j, beta * value) for part, j, value in found] for found in along_terms(slot, rim, bond_edge)]
        for side in range(2):
            for part, j, value in terms[side]:
                rim_send[other, 1 - side, spot(part, j)] += value
        more = n < ITERS - 3

        @pl.when(more)
        def _():
            send_rim(other)

        def put(part, r, at, value):
            pull[part, r, at : at + 1, :] += value
            field[other, part, 3 + r, PAD + at : PAD + at + 1, :] += value

        spread(terms, put)

        @pl.when(more)
        def _():
            send_all(other, across)

        advance(alpha, beta, slot)
        products(n + 2, other, False)
        return alpha, beta

    one = jnp.ones((8, DEPTH), F32)
    alpha, beta = lax.fori_loop(0, ITERS - 2, cycle, (one, jnp.zeros((8, DEPTH), F32)))
    sum_middle(ITERS - 1)
    alpha, beta = damping_of(ITERS - 2, alpha, beta)
    advance(alpha, beta, (ITERS - 2) % 2)
    alpha, beta = damping_of(ITERS - 1, alpha, beta)

    def finish(r, carry):
        for part in range(3):
            for t in range(2):
                at = (part, r, pl.ds(8 * t, 8), slice(None))
                v = alpha * v_out[at] + beta * total[at]
                v_out[at] = v
                u_out[at] = u_out[at] + v
        return carry

    lax.fori_loop(0, ROWS, finish, 0)


def on_device(nx, ny, disp, vel, load, flags, mask_bits):
    block = (3, ROWS, COLS, DEPTH)
    any_spec = pl.BlockSpec(memory_space=pl.ANY)
    vmem_spec = pl.BlockSpec(memory_space=pltpu.VMEM)
    turns = ITERS
    dma = pltpu.SemaphoreType.DMA
    scratch = [
        pltpu.VMEM((SLOTS, 3, TALL, WIDE, DEPTH), F32),
        pltpu.VMEM((SLOTS, 2, 3, 2, WIDE, DEPTH), F32),
        pltpu.VMEM((SLOTS, 2, WIDE, DEPTH), F32),
        pltpu.VMEM((SLOTS, 2, 7, 24, DEPTH), F32),
        pltpu.VMEM((SLOTS, 4, 16, DEPTH), F32),
        pltpu.VMEM((SLOTS, 2, 7, 8, DEPTH), F32),
        pltpu.VMEM((SLOTS, 4, 16, DEPTH), F32),
        pltpu.VMEM((4, TALL, WIDE, DEPTH), I32),
        pltpu.VMEM((2, 4, 3, WIDE, DEPTH), I32),
        pltpu.VMEM((2, 4, 3, 24, DEPTH), I32),
        pltpu.VMEM((4, 16, DEPTH), I32),
        pltpu.VMEM((2, 4, 3, 8, DEPTH), I32),
        pltpu.VMEM((4, 16, DEPTH), I32),
        pltpu.VMEM((BONDS, ROWS * COLS, DEPTH), F32),
        pltpu.VMEM((2, len(EDGE), ROWS, DEPTH), F32),
        pltpu.VMEM((6, ROWS, COLS, DEPTH), F32),
        pltpu.VMEM((4,) + block, F32),
        pltpu.VMEM(block, F32),
        pltpu.VMEM(block[1:], I32),
        pltpu.VMEM((turns, nx, 1, DEPTH), F32),
        pltpu.VMEM((turns, ny, 1, DEPTH), F32),
        dma((7,)),
        dma((SLOTS, 10)),
        dma((SLOTS, 10)),
        dma((8,)),
        dma((8,)),
        dma((2, turns)),
        dma((2, turns)),
    ]
    return pl.pallas_call(
        functools.partial(kernel, nx, ny),
        out_shape=[pltpu.VMEM(block, F32)] * 2,
        in_specs=[any_spec] * 5,
        out_specs=[vmem_spec] * 2,
        scratch_shapes=scratch,
        compiler_params=pltpu.CompilerParams(
            collective_id=0, has_side_effects=True, vmem_limit_bytes=60_000_000
        ),
    )(disp, vel, load, flags, mask_bits)


def solution(mesh):
    split = P(None, "gx", "gy", None)
    return jax.shard_map(
        functools.partial(on_device, mesh.shape["gx"], mesh.shape["gy"]),
        mesh=mesh,
        in_specs=(split, split, split, P("gx", "gy", None), split),
        out_specs=(split, split),
        check_vma=False,
    )
```

```python
import functools
import math

import jax
import jax.numpy as jnp
from jax import lax
from jax.experimental import pallas as pl
from jax.experimental.pallas import tpu as pltpu
from jax.sharding import PartitionSpec as P

ITERS = 8
MASS = 64.0
EPSILON = 1e-06
ROWS = 8
COLS = 16
DEPTH = 128
PAD = 8
WIDE = COLS + 2 * PAD
TALL = ROWS + 6
GROUP = 4
SLOTS = 4
F32 = jnp.float32
I32 = jnp.int32


def neighbour_table():
    table = []
    for across in range(-3, 4):
        for along in range(-3, 4):
            for upward in range(-3, 4):
                length = across * across + along * along + upward * upward
                if 0 < length <= 9:
                    table.append((across, along, upward))
    return table


TABLE = neighbour_table()
NUMBER = {offset: k for k, offset in enumerate(TABLE)}
BONDS = len(TABLE)


def on_axis(offset):
    return sum(1 for part in offset if part) == 1


def weight_of(offset):
    length = float(sum(part * part for part in offset))
    weight = 1.0 / (length * math.sqrt(length))
    return weight * length if on_axis(offset) else weight


def oblique(b, c):
    return [a for a in range(-2, 3) if (a, b, c) in NUMBER and not on_axis((a, b, c))]


EDGE = []
for _c in range(-2, 3):
    for _reach in (1, 2, 3):
        for _a in range(-2, 3):
            if (_a, _reach, _c) in NUMBER:
                for _j in range(_reach):
                    EDGE.append((_a, _reach, _c, _j, _reach - 1 - _j))
EDGE_AT = {entry[:4]: n for n, entry in enumerate(EDGE)}


def add(total, term):
    return term if total is None else total + term


def sub(total, term):
    return -term if total is None else total - term


def scaled(factor, value):
    if factor == 1:
        return value
    if factor == -1:
        return -value
    return float(factor) * value


def plus_scaled(total, factor, value):
    if total is None:
        return scaled(factor, value)
    if factor == 1:
        return total + value
    if factor == -1:
        return total - value
    return total + float(factor) * value


def combine(weights, totals):
    out = None
    for factor, value in zip(weights, totals):
        if factor and value is not None:
            out = plus_scaled(out, factor, value)
    return out


def accumulate_first(total, factor, value):
    if factor == 0 or value is None:
        return total
    if factor == 2:
        return value
    if factor == -2:
        return 2.0 * (total - value)
    return plus_scaled(total, factor, value)


def turned(value, c):
    if c == 0:
        return value
    return pltpu.roll(value, (-c) % DEPTH, 1)


def moments(terms):
    zeroth = None
    for a in sorted(terms):
        zeroth = add(zeroth, terms[a])
    first = None
    if 2 in terms:
        first = add(first, terms[2])
    if -2 in terms:
        first = sub(first, terms[-2])
    if first is not None:
        first = 2.0 * first
    if 1 in terms:
        first = add(first, terms[1])
    if -1 in terms:
        first = sub(first, terms[-1])
    return zeroth, first


def local_pass(slot, field, bond, diag, out):
    def group(g, carry):
        base = g * GROUP
        for t in range(2):
            col = PAD + 8 * t

            def coef(offset, i):
                start = pl.multiple_of((base + i) * COLS + 8 * t, 8)
                return bond[NUMBER[offset], pl.ds(start, 8), :]

            def source(part, i, b):
                return field[slot, part, base + 3 + i, pl.ds(col + b, 8), :]

            for c in (0, 1, -1, 2, -2, 3, -3):
                g0 = [None] * GROUP
                g1 = [None] * GROUP
                g2 = [None] * GROUP
                if c:
                    for i in range(GROUP):
                        g2[i] = coef((0, 0, c), i) * source(2, i, 0)
                if c == 0:
                    for i in range(GROUP):
                        for a in (1, -1, 2, -2, 3, -3):
                            g0[i] = add(g0[i], coef((a, 0, 0), i) * source(0, i + a, 0))
                        for b in (1, -1, 2, -2, 3, -3):
                            g1[i] = add(g1[i], coef((0, b, 0), i) * source(1, i, b))
                if abs(c) < 3:
                    n0 = [None] * GROUP
                    n1 = [None] * GROUP
                    for b in (2, -2, 1, -1, 0):
                        reach = oblique(b, c)
                        if not reach:
                            continue
                        span = range(min(reach), GROUP + max(reach))
                        u0 = {i: source(0, i, b) for i in span}
                        twice = {i: 2.0 * u0[i] for i in span} if 2 in reach else None
                        u1 = {i: source(1, i, b) if b else None for i in span}
                        u2 = {i: source(2, i, b) if c else None for i in span}
                        s = {i: combine((b, c), (u1[i], u2[i])) for i in span}
                        for i in range(GROUP):
                            terms = {}
                            for a in reach:
                                near = s[i + a]
                                if abs(a) == 1:
                                    near = near + u0[i + a] if a > 0 else near - u0[i + a]
                                elif a:
                                    near = near + twice[i + a] if a > 0 else near - twice[i + a]
                                terms[a] = coef((a, b, c), i) * near
                            zeroth, first = moments(terms)
                            g0[i] = add(g0[i], first)
                            if c:
                                n0[i] = add(n0[i], zeroth)
                            if b == 2:
                                n1[i] = zeroth
                            elif b == -2:
                                n1[i] = 2.0 * (n1[i] - zeroth)
                            elif b:
                                n1[i] = plus_scaled(n1[i], b, zeroth)
                    for i in range(GROUP):
                        g1[i] = add(g1[i], n1[i])
                        if c:
                            g2[i] = plus_scaled(g2[i], c, n0[i])
                for i in range(GROUP):
                    for part, value in enumerate((g0[i], g1[i], g2[i])):
                        if c == 0:
                            if diag is not None:
                                u = [source(other, i, 0) for other in range(3)]
                                value = less_diagonal(value, diag, part, base + i, t, u)
                            elif value is None:
                                value = jnp.zeros((8, DEPTH), F32)
                            out[part, base + i, pl.ds(8 * t, 8), :] = value
                        elif value is not None:
                            out[part, base + i, pl.ds(8 * t, 8), :] += turned(value, c)
        return carry

    lax.fori_loop(0, ROWS // GROUP, group, 0)


def less_diagonal(value, diag, part, r, t, u):
    own = None
    for other in range(3):
        pair = DIAG[min(part, other), max(part, other)]
        own = add(own, diag[pair, r, pl.ds(8 * t, 8), :] * u[other])
    return -own if value is None else value - own


DIAG = {(0, 0): 0, (0, 1): 1, (1, 1): 2, (0, 2): 3, (1, 2): 4, (2, 2): 5}


def across_pass(slot, near, far, bond, out):
    for side in range(2):
        sign = 1 if side else -1
        edge = ROWS - 1 if side else 0
        for t in range(2):
            col = PAD + 8 * t

            def coef(offset, i):
                return bond[NUMBER[offset], pl.ds((edge - sign * i) * COLS + 8 * t, 8), :]

            def source(part, layer, b):
                e = layer if side else 1 - layer
                return near[slot, side, part, e, pl.ds(col + b, 8), :]

            sums = [[None] * 3 for i in range(2)]
            third = None
            for c in (0, 1, -1, 2, -2):
                g = [[None] * 3 for i in range(2)]
                if c == 0:
                    for layer in range(2):
                        u0 = source(0, layer, 0)
                        for i in range(3):
                            a = sign * (i + layer + 1)
                            if abs(a) <= 3:
                                term = coef((a, 0, 0), i) * u0
                                if i < 2:
                                    g[i][0] = add(g[i][0], term)
                                else:
                                    third = term
                    g[0][0] = g[0][0] + coef((3 * sign, 0, 0), 0) * far[slot, side, pl.ds(col, 8), :]
                n0 = [None] * 2
                n1 = [None] * 2
                deep = [None] * 2
                for b in (2, -2, 1, -1, 0):
                    reach = oblique(b, c)
                    if not reach:
                        continue
                    zeroth = [None] * 2
                    for layer in range(max(reach)):
                        u0 = source(0, layer, b)
                        u1 = source(1, layer, b) if b else None
                        u2 = source(2, layer, b) if c else None
                        s = combine((b, c), (u1, u2))
                        for i in range(2):
                            size = i + layer + 1
                            a = sign * size
                            if a not in reach:
                                continue
                            if size == 2 and i == 1:
                                q = plus_scaled(q, sign, u0)
                            else:
                                q = plus_scaled(s, a, u0)
                            term = coef((a, b, c), i) * q
                            zeroth[i] = add(zeroth[i], term)
                            if size == 1:
                                g[i][0] = plus_scaled(g[i][0], sign, term)
                            else:
                                deep[i] = add(deep[i], term)
                    for i in range(2):
                        if zeroth[i] is None:
                            continue
                        if c:
                            n0[i] = add(n0[i], zeroth[i])
                        n1[i] = accumulate_first(n1[i], b, zeroth[i])
                for i in range(2):
                    if deep[i] is not None:
                        g[i][0] = plus_scaled(g[i][0], 2 * sign, deep[i])
                for i in range(2):
                    g[i][1] = n1[i]
                    g[i][2] = scaled(c, n0[i]) if c else None
                    for part in range(3):
                        if g[i][part] is not None:
                            sums[i][part] = add(sums[i][part], turned(g[i][part], c))
            for i in range(2):
                row = edge - sign * i
                for part in range(3):
                    out[part, row, pl.ds(8 * t, 8), :] += sums[i][part]
            out[0, edge - 2 * sign, pl.ds(8 * t, 8), :] += third


def along_terms(slot, rim, bond_edge):
    found = []
    for side in range(2):
        sign = 1 if side else -1

        def coef(a, size, c, j):
            return bond_edge[side, EDGE_AT[a, size, c, j]]

        def source(part, layer, a):
            return rim[slot, side, part * 2 + layer, pl.ds(8 + a, 8), :]

        sums = [[None] * 3 for j in range(2)]
        third = None
        for c in (0, 1, -1, 2, -2):
            g = [[None] * 3 for j in range(2)]
            if c == 0:
                for layer in range(3):
                    at = 6 if layer == 2 else 2 + layer
                    u1 = rim[slot, side, at, pl.ds(8, 8), :]
                    for j in range(3 - layer):
                        term = coef(0, layer + 1 + j, 0, j) * u1
                        if j < 2:
                            g[j][1] = add(g[j][1], term)
                        else:
                            third = term
            n0 = [None] * 2
            n1 = [None] * 2
            deep = [None] * 2
            for a in (2, -2, 1, -1, 0):
                reach = [size for size in (1, 2) if (a, size, c) in NUMBER and not on_axis((a, size, c))]
                if not reach:
                    continue
                zeroth = [None] * 2
                for layer in range(max(reach)):
                    u0 = source(0, layer, a) if a else None
                    u1 = source(1, layer, a)
                    u2 = source(2, layer, a) if c else None
                    s = combine((a, c), (u0, u2))
                    for j in range(2):
                        size = j + layer + 1
                        if size not in reach:
                            continue
                        if size == 2 and j == 1:
                            q = plus_scaled(q, sign, u1)
                        else:
                            q = plus_scaled(s, sign * size, u1)
                        term = coef(a, size, c, j) * q
                        zeroth[j] = add(zeroth[j], term)
                        if size == 1:
                            g[j][1] = plus_scaled(g[j][1], sign, term)
                        else:
                            deep[j] = add(deep[j], term)
                for j in range(2):
                    if zeroth[j] is None:
                        continue
                    if c:
                        n0[j] = add(n0[j], zeroth[j])
                    n1[j] = accumulate_first(n1[j], a, zeroth[j])
            for j in range(2):
                if deep[j] is not None:
                    g[j][1] = plus_scaled(g[j][1], 2 * sign, deep[j])
            for j in range(2):
                g[j][0] = n1[j]
                g[j][2] = scaled(c, n0[j]) if c else None
                for part in range(3):
                    if g[j][part] is not None:
                        sums[j][part] = add(sums[j][part], turned(g[j][part], c))
        found.append([(part, j, sums[j][part]) for part in range(3) for j in range(2)] + [(1, 2, third)])
    return found


def spread(found, put):
    for side in range(2):
        for part, j, value in found[side]:
            at = COLS - 1 - j if side else j
            for r in range(ROWS):
                put(part, r, at, value[r : r + 1, :])


def weight_if_intact(near, far, offset):
    k = NUMBER[offset]
    word, bit = divmod(k, 31)
    far_word, far_bit = divmod(BONDS - 1 - k, 31)
    broken = (near[word] & I32(1 << bit)) | (far(far_word) & I32(1 << far_bit))
    return jnp.where(broken == 0, F32(weight_of(offset)), F32(0.0))


def moved(own, c):
    if not c:
        return own
    lane = lax.broadcasted_iota(I32, (8, DEPTH), 1)
    outside = lane < c if c > 0 else lane >= DEPTH + c
    return [jnp.where(outside, I32(-1), pltpu.roll(word, c % DEPTH, 1)) for word in own]


def tally(sums, offset, value):
    a, b, c = offset
    if on_axis(offset):
        at = 0 if a else (2 if b else 5)
        sums[at] = add(sums[at], value)
        return
    for at, factor in enumerate((a * a, a * b, b * b, a * c, b * c, c * c)):
        if factor:
            sums[at] = plus_scaled(sums[at], factor, value)


def build_bonds(words, bond, diag):
    def row(r, carry):
        for t in range(2):
            start = pl.multiple_of(r * COLS + 8 * t, 8)
            own = [words[w, r + 3, pl.ds(PAD + 8 * t, 8), :] for w in range(4)]
            totals = [None] * 6
            for c in range(-3, 4):
                near = moved(own, c)
                sums = [None] * 6
                for b in range(-3, 4):
                    values = {}
                    for a in range(-3, 4):
                        k = NUMBER.get((a, b, c))
                        if k is None:
                            continue

                        def far(w):
                            return words[w, r + 3 + a, pl.ds(PAD + 8 * t + b, 8), :]

                        value = weight_if_intact(near, far, (a, b, c))
                        bond[k, pl.ds(start, 8), :] = value
                        if on_axis((a, b, c)):
                            tally(sums, (a, b, c), value)
                        else:
                            values[a] = value
                    if not values:
                        continue
                    zeroth, first = moments(values)
                    second = None
                    if 2 in values:
                        second = 4.0 * (values[2] + values[-2])
                    second = add(second, values[1] + values[-1])
                    sums[0] = add(sums[0], second)
                    if b:
                        sums[1] = plus_scaled(sums[1], b, first)
                        sums[2] = plus_scaled(sums[2], b * b, zeroth)
                    if c:
                        sums[3] = plus_scaled(sums[3], c, first)
                        sums[5] = plus_scaled(sums[5], c * c, zeroth)
                        if b:
                            sums[4] = plus_scaled(sums[4], b * c, zeroth)
                for n in range(6):
                    if sums[n] is not None:
                        totals[n] = add(totals[n], turned(sums[n], c))
            for n in range(6):
                diag[n, r, pl.ds(8 * t, 8), :] = totals[n]
        return carry

    lax.fori_loop(0, ROWS, row, 0)


def build_across(words, words_near, bond, diag):
    for side in range(2):
        sign = 1 if side else -1
        edge = ROWS - 1 if side else 0
        for t in range(2):
            for i in range(3):
                r = edge - sign * i
                own = [words[w, r + 3, pl.ds(PAD + 8 * t, 8), :] for w in range(4)]
                totals = [None] * 6
                for c in range(-2, 3):
                    if i == 2 and c:
                        continue
                    near = moved(own, c)
                    sums = [None] * 6
                    for b in range(-2, 3):
                        for layer in range(3 - i):
                            offset = (sign * (i + layer + 1), b, c)
                            if offset not in NUMBER:
                                continue

                            def far(w):
                                e = layer if side else 2 - layer
                                return words_near[side, w, e, pl.ds(PAD + 8 * t + b, 8), :]

                            value = weight_if_intact(near, far, offset)
                            bond[NUMBER[offset], pl.ds(r * COLS + 8 * t, 8), :] = value
                            tally(sums, offset, value)
                    for n in range(6):
                        if sums[n] is not None:
                            totals[n] = add(totals[n], turned(sums[n], c))
                for n in range(6):
                    if totals[n] is not None:
                        diag[n, r, pl.ds(8 * t, 8), :] += totals[n]


def build_along(words_mine, words_rim, bond_edge, diag):
    for side in range(2):
        sign = 1 if side else -1
        edge = COLS - 1 if side else 0
        for j in range(3):
            own = [words_mine[1 - side, w, j] for w in range(4)]
            totals = [None] * 6
            for c in range(-2, 3):
                if j == 2 and c:
                    continue
                near = moved(own, c)
                sums = [None] * 6
                for n, (a, size, up, col, layer) in enumerate(EDGE):
                    if col != j or up != c:
                        continue
                    offset = (a, sign * size, c)

                    def far(w):
                        return words_rim[side, w, layer, pl.ds(8 + a, 8), :]

                    value = weight_if_intact(near, far, offset)
                    bond_edge[side, n] = value
                    tally(sums, offset, value)
                for n in range(6):
                    if sums[n] is not None:
                        totals[n] = add(totals[n], turned(sums[n], c))
            at = edge - sign * j
            for n in range(6):
                if totals[n] is not None:
                    for r in range(ROWS):
                        diag[n, r, at : at + 1, :] += totals[n][r : r + 1, :]


def kernel(
    nx, ny,
    disp, vel, load, flags, mask,
    u_out, v_out, t_out, a_out, b_out,
    field, near, far, rim, corner, rim_send, corner_send,
    words, words_near, words_rim, words_corner, words_rim_send, words_corner_send,
    bond, bond_edge, diag,
    pool, load_buf, flag_buf,
    ring_one, ring_two,
    in_sem, send_sem, recv_sem, word_send, word_recv, sum_send, sum_recv,
):
    total, rate, force, pull = (pool.at[n] for n in range(4))
    ax = lax.axis_index("gx")
    ay = lax.axis_index("gy")
    here = {-1: (ax > 0, ay > 0), 1: (ax < nx - 1, ay < ny - 1)}

    def exists(dx, dy):
        cond = None
        if dx:
            cond = here[dx][0]
        if dy:
            other = here[dy][1]
            cond = other if cond is None else cond & other
        return cond

    def device(dx, dy):
        return {"gx": ax + dx, "gy": ay + dy}

    sides = [(dx, dy) for dx in (-1, 0, 1) for dy in (-1, 0, 1) if dx or dy]
    diagonals = [(dx, dy) for dx, dy in sides if dx and dy]

    own_rows = pl.ds(3, ROWS)
    own_cols = pl.ds(PAD, COLS)
    loads = [
        pltpu.make_async_copy(mask, words.at[:, own_rows, own_cols], in_sem.at[0]),
        pltpu.make_async_copy(vel, field.at[1, :, own_rows, own_cols], in_sem.at[1]),
        pltpu.make_async_copy(disp, field.at[0, :, own_rows, own_cols], in_sem.at[2]),
        pltpu.make_async_copy(disp, u_out, in_sem.at[3]),
        pltpu.make_async_copy(vel, v_out, in_sem.at[4]),
        pltpu.make_async_copy(load, load_buf, in_sem.at[5]),
        pltpu.make_async_copy(flags, flag_buf, in_sem.at[6]),
    ]
    for copy in loads:
        copy.start()

    zero8 = jnp.zeros((8, DEPTH), F32)

    barrier = pltpu.get_barrier_semaphore()
    for step in range(1, nx):
        pl.semaphore_signal(barrier, inc=1, device_id={"gx": lax.rem(ax + step, nx), "gy": ay})
    for step in range(1, ny):
        pl.semaphore_signal(barrier, inc=1, device_id={"gx": ax, "gy": lax.rem(ay + step, ny)})
    for dx, dy in diagonals:
        where = {"gx": lax.rem(ax + dx + nx, nx), "gy": lax.rem(ay + dy + ny, ny)}
        pl.semaphore_signal(barrier, inc=1, device_id=where)


    inner = slice(PAD, PAD + COLS)
    pads = (slice(0, PAD), slice(PAD + COLS, WIDE))
    borders = list(range(3)) + list(range(TALL - 3, TALL))

    def broken(*shape):
        return jnp.full(shape + (DEPTH,), -1, I32)

    def clear():
        def slot_clear(slot, carry):
            for part in range(3):
                for r in borders:
                    field[slot, part, r] = jnp.zeros((WIDE, DEPTH), F32)
                for r in range(3, TALL - 3):
                    for pad in pads:
                        field[slot, part, r, pad, :] = zero8
                for side in range(2):
                    for e in range(2):
                        for pad in pads:
                            near[slot, side, part, e, pad, :] = zero8
            for side in range(2):
                for at in range(7):
                    rim[slot, side, at, 0:8, :] = zero8
                    rim[slot, side, at, 16:24, :] = zero8
            return carry

        lax.fori_loop(0, SLOTS, slot_clear, 0)
        for w in range(4):
            for r in range(TALL):
                if r in borders:
                    words[w, r] = broken(WIDE)
                else:
                    for pad in pads:
                        words[w, r, pad, :] = broken(PAD)
            for side in range(2):
                for layer in range(3):
                    for pad in pads:
                        words_near[side, w, layer, pad, :] = broken(PAD)
                    words_rim[side, w, layer, 0:8, :] = broken(8)
                    words_rim[side, w, layer, 16:24, :] = broken(8)
        for side in range(2):
            @pl.when(ax == (nx - 1 if side else 0))
            def _():
                for slot in range(SLOTS):
                    far[slot, side, inner, :] = jnp.zeros((COLS, DEPTH), F32)
                    for part in range(3):
                        for e in range(2):
                            near[slot, side, part, e, inner, :] = jnp.zeros((COLS, DEPTH), F32)
                for w in range(4):
                    for layer in range(3):
                        words_near[side, w, layer, inner, :] = broken(COLS)

            @pl.when(ay == (ny - 1 if side else 0))
            def _():
                for slot in range(SLOTS):
                    for at in range(7):
                        rim[slot, side, at, 8:16, :] = zero8
                for w in range(4):
                    for layer in range(3):
                        words_rim[side, w, layer, 8:16, :] = broken(8)

    def edge_rows(dx):
        return (0, 2) if dx < 0 else (ROWS - 2, ROWS - 3)

    def halo_copies(slot, dx, dy):
        into = {-1: 1, 1: 0}
        if dx and dy:
            n = into[dx] * 2 + into[dy]
            return [(corner_send.at[slot, n], corner.at[slot, n], 6 + n)]
        if dx:
            first, third = edge_rows(dx)
            side = into[dx]
            return [
                (
                    field.at[slot, :, pl.ds(3 + first, 2), own_cols],
                    near.at[slot, side, :, :, own_cols],
                    side,
                ),
                (field.at[slot, 0, 3 + third, own_cols], far.at[slot, side, own_cols], 2 + side),
            ]
        side = into[dy]
        return [(rim_send.at[slot, side], rim.at[slot, side, :, pl.ds(8, 8)], 4 + side)]

    def spot(part, layer):
        return 6 if layer == 2 else part * 2 + layer

    def pack_rim(slot):
        for side in range(2):
            for part in range(3):
                for layer in range(3 if part == 1 else 2):
                    col = PAD + (layer if side else COLS - 1 - layer)
                    for r in range(ROWS):
                        rim_send[slot, side, spot(part, layer), r : r + 1, :] = field[
                            slot, part, 3 + r, col : col + 1, :
                        ]

    def ends(dx):
        return slice(0, 2) if dx < 0 else slice(ROWS - 2, ROWS)

    def beyond(dx):
        return slice(6, 8) if dx < 0 else slice(16, 18)

    def copy_of(slot, dx, dy, src, dst, n):
        return pltpu.make_async_remote_copy(
            src_ref=src, dst_ref=dst, send_sem=send_sem.at[slot, n], recv_sem=recv_sem.at[slot, n],
            device_id=device(dx, dy),
        )

    along = [(0, -1), (0, 1)]
    across = [(-1, 0), (1, 0)]

    def send_all(slot, which):
        for dx, dy in which:
            @pl.when(exists(dx, dy))
            def _():
                for src, dst, n in halo_copies(slot, dx, dy):
                    copy_of(slot, dx, dy, src, dst, n).start()

    def send_rim(slot):
        send_all(slot, along)
        for dx, dy in diagonals:
            n = (1 if dx < 0 else 0) * 2 + (1 if dy < 0 else 0)
            for at in range(6):
                corner_send[slot, n, 2 * at : 2 * at + 2, :] = rim_send[slot, 1 if dy < 0 else 0, at, ends(dx), :]
        send_all(slot, diagonals)

    def halo_send(slot):
        pack_rim(slot)
        send_rim(slot)
        send_all(slot, across)

    def wait_all(slot, which):
        for dx, dy in which:
            @pl.when(exists(dx, dy))
            def _():
                for src, dst, n in halo_copies(slot, dx, dy):
                    copy_of(slot, dx, dy, src, dst, n).wait_send()
                for src, dst, n in halo_copies(slot, -dx, -dy):
                    copy_of(slot, dx, dy, src, dst, n).wait_recv()

    def wait_rim(slot):
        wait_all(slot, along + diagonals)
        for dx, dy in diagonals:
            sx, sy = (1 if dx > 0 else 0), (1 if dy > 0 else 0)

            @pl.when(exists(dx, dy))
            def _():
                for at in range(6):
                    rim[slot, sy, at, beyond(dx), :] = corner[slot, sx * 2 + sy, 2 * at : 2 * at + 2, :]

    def word_copies(dx, dy):
        into = {-1: 1, 1: 0}
        if dx and dy:
            n = into[dx] * 2 + into[dy]
            return [(words_corner_send.at[n], words_corner.at[n], 4 + n)]
        if dx:
            side = into[dx]
            first, third = edge_rows(dx)
            two, one = (pl.ds(0, 2), 2) if side else (pl.ds(1, 2), 0)
            w = third_word((3, 0, 0), side)
            return [
                (words.at[:, pl.ds(3 + first, 2), own_cols], words_near.at[side, :, two, own_cols], side),
                (words.at[w, 3 + third, own_cols], words_near.at[side, w, one, own_cols], 8 + side),
            ]
        side = into[dy]
        w = third_word((0, 3, 0), side)
        two = pl.ds(0, 2)
        return [
            (words_rim_send.at[side, :, two], words_rim.at[side, :, two, pl.ds(8, 8)], 2 + side),
            (words_rim_send.at[side, w, 2], words_rim.at[side, w, 2, pl.ds(8, 8)], 10 + side),
        ]

    def third_word(offset, side):
        if not side:
            offset = tuple(-part for part in offset)
        return (BONDS - 1 - NUMBER[offset]) // 31

    def word_copy(dx, dy, src, dst, n):
        return pltpu.make_async_remote_copy(
            src_ref=src, dst_ref=dst, send_sem=word_send.at[n], recv_sem=word_recv.at[n], device_id=device(dx, dy),
        )

    loads[0].wait()
    for side in range(2):
        for w in range(4):
            for layer in range(3):
                col = PAD + (layer if side else COLS - 1 - layer)
                for r in range(ROWS):
                    words_rim_send[side, w, layer, r : r + 1, :] = words[w, 3 + r, col : col + 1, :]
    for dx, dy in diagonals:
        n = (1 if dx < 0 else 0) * 2 + (1 if dy < 0 else 0)
        for w in range(4):
            for layer in range(2):
                at = (w * 2 + layer) * 2
                words_corner_send[n, at : at + 2, :] = words_rim_send[1 if dy < 0 else 0, w, layer, ends(dx), :]
    pl.semaphore_wait(barrier, nx + ny + 2)
    for dx, dy in sides:
        @pl.when(exists(dx, dy))
        def _():
            for src, dst, n in word_copies(dx, dy):
                word_copy(dx, dy, src, dst, n).start()
    loads[2].wait()
    halo_send(0)

    clear()
    build_bonds(words, bond, diag)
    loads[1].wait()
    halo_send(1)
    def words_wait():
        for dx, dy in sides:
            @pl.when(exists(dx, dy))
            def _():
                for src, dst, n in word_copies(dx, dy):
                    word_copy(dx, dy, src, dst, n).wait_send()
                for src, dst, n in word_copies(-dx, -dy):
                    word_copy(dx, dy, src, dst, n).wait_recv()
        for dx, dy in diagonals:
            sx, sy = (1 if dx > 0 else 0), (1 if dy > 0 else 0)

            @pl.when(exists(dx, dy))
            def _():
                for w in range(4):
                    for layer in range(2):
                        at = (w * 2 + layer) * 2
                        words_rim[sy, w, layer, beyond(dx), :] = words_corner[sx * 2 + sy, at : at + 2, :]

        build_across(words, words_near, bond, diag)
        build_along(words_rim_send, words_rim, bond_edge, diag)

    def sum_copy(src, dst, which, turn, where):
        return pltpu.make_async_remote_copy(
            src_ref=src, dst_ref=dst, send_sem=sum_send.at[which, turn], recv_sem=sum_recv.at[which, turn],
            device_id=where,
        )

    def sum_begin(turn, rows):
        slab = jnp.concatenate([jnp.sum(row, axis=0, keepdims=True) for row in rows] + [jnp.zeros((2, DEPTH), F32)], axis=0)
        each = jnp.broadcast_to(jnp.sum(slab, axis=1, keepdims=True), (8, DEPTH))
        mine = lax.broadcasted_iota(I32, (8, DEPTH), 0) == lax.broadcasted_iota(I32, (8, DEPTH), 1)
        ring_one[turn, ax] = jnp.sum(jnp.where(mine, each, 0.0), axis=0, keepdims=True)
        for step in range(1, nx):
            sum_copy(
                ring_one.at[turn, ax], ring_one.at[turn, ax], 0, turn, {"gx": lax.rem(ax + step, nx), "gy": ay}
            ).start()

    def sum_middle(turn):
        some = ring_one.at[turn, pl.ds(0, nx - 1)]
        copy = sum_copy(some, some, 0, turn, {"gx": ax, "gy": ay})
        copy.wait_recv()
        copy.wait_send()
        ring_two[turn, ay] = jnp.sum(ring_one[turn], axis=0)
        for step in range(1, ny):
            sum_copy(
                ring_two.at[turn, ay], ring_two.at[turn, ay], 1, turn, {"gx": ax, "gy": lax.rem(ay + step, ny)}
            ).start()

    def sum_end(turn):
        some = ring_two.at[turn, pl.ds(0, ny - 1)]
        copy = sum_copy(some, some, 1, turn, {"gx": ax, "gy": ay})
        copy.wait_recv()
        copy.wait_send()
        row = jnp.sum(ring_two[turn], axis=0)
        return [jnp.broadcast_to(row[:, n : n + 1], (8, DEPTH)) for n in range(6)]

    count = 3.0 * ROWS * nx * COLS * ny * DEPTH

    def damping_of(turn, alpha, beta):
        g0, g1, g2, h0, h1, h2 = sum_end(turn)
        kinetic = alpha * alpha * g0 + 2.0 * alpha * beta * g1 + beta * beta * g2
        rayleigh = -(alpha * alpha * h0 + 2.0 * alpha * beta * h1 + beta * beta * h2)
        rayleigh = jnp.maximum(rayleigh, 0.0)
        damping = 2.0 * jnp.sqrt((rayleigh / count) / (MASS * (kinetic / count + EPSILON)))
        return (2.0 - damping) / (2.0 + damping), 2.0 / (MASS * (2.0 + damping))

    def own(ref_slot, part, r, t):
        return field[ref_slot, part, 3 + r, pl.ds(PAD + 8 * t, 8), :]

    vregs = [(part, r, t) for part in range(3) for r in range(ROWS) for t in range(2)]

    def tally_pair(acc, v, t, w):
        return (acc[0] + v * v, acc[1] + v * t, acc[2] + t * t, acc[3] + v * w, acc[4] + t * w)

    def early_products():
        def body(r, acc):
            for part in range(3):
                for t in range(2):
                    at = (part, r, pl.ds(8 * t, 8), slice(None))
                    acc = tally_pair(acc, v_out[at], total[at], rate[at])
            return acc

        return lax.fori_loop(0, ROWS, body, (zero8,) * 5)

    def late_product(slot):
        def body(r, acc):
            acc = list(acc)
            for part in range(3):
                for t in range(2):
                    acc[t] = acc[t] + total[part, r, pl.ds(8 * t, 8), :] * own(slot, part, r, t)
            return tuple(acc)

        acc = lax.fori_loop(0, ROWS, body, (zero8,) * 2)
        return acc[0] + acc[1]

    def rest(slot, out):
        wait_all(slot, across)
        across_pass(slot, near, far, bond, out)
        wait_rim(slot)

        def put(part, r, at, value):
            out[part, r, at : at + 1, :] += value

        spread(along_terms(slot, rim, bond_edge), put)

    for copy in loads[3:]:
        copy.wait()

    def begin(n, carry):
        out = pool.at[n]
        local_pass(n, field, bond, None, out)

        @pl.when(n == 0)
        def _():
            words_wait()

        rest(n, out)
        loaded = lax.div(3 - n, 3).astype(F32)
        to = lax.rem(n + 2, 4)

        def put(r, carry):
            for t in range(2):
                at = (r, pl.ds(8 * t, 8), slice(None))
                active = loaded * flag_buf[at].astype(F32)
                u = [own(n, part, r, t) for part in range(3)]
                for part in range(3):
                    value = less_diagonal(out[(part,) + at], diag, part, r, t, u)
                    value = value + active * load_buf[(part,) + at]
                    out[(part,) + at] = value
                    field[to, part, 3 + r, pl.ds(PAD + 8 * t, 8), :] = value
            return carry

        lax.fori_loop(0, ROWS, put, 0)

        @pl.when(n < 3)
        def _():
            halo_send(to)

        @pl.when(n == 1)
        def _():
            sum_begin(0, early_products() + (zero8,))

        @pl.when(n == 2)
        def _():
            sum_middle(0)
            sum_begin(1, early_products() + (late_product(0),))

        return carry

    lax.fori_loop(0, 4, begin, 0)

    def advance(alpha, beta, slot):
        def body(r, acc):
            for part in range(3):
                for t in range(2):
                    at = (part, r, pl.ds(8 * t, 8), slice(None))
                    v, tt, w, y = v_out[at], total[at], rate[at], own(slot, part, r, t)
                    v = alpha * v + beta * tt
                    w = alpha * w + beta * y
                    tt = tt + w
                    v_out[at] = v
                    u_out[at] = u_out[at] + v
                    rate[at] = w
                    total[at] = tt
                    acc = tally_pair(acc, v, tt, w)
            return acc

        return lax.fori_loop(0, ROWS, body, (zero8,) * 5)

    def cycle(n, carry):
        alpha, beta = carry
        slot = lax.rem(n, 2)
        other = 1 - slot
        local_pass(slot, field, bond, diag, force)
        wait_all(slot, across)
        across_pass(slot, near, far, bond, force)
        sum_middle(n + 1)
        alpha, beta = damping_of(n, alpha, beta)

        def body(r, carry):
            for part in range(3):
                for t in range(2):
                    at = (part, r, pl.ds(8 * t, 8), slice(None))
                    x = alpha * pull[at] + beta * force[at]
                    pull[at] = x
                    field[other, part, 3 + r, pl.ds(PAD + 8 * t, 8), :] = own(slot, part, r, t) + x
            return carry

        lax.fori_loop(0, ROWS, body, 0)
        pack_rim(other)
        early = advance(alpha, beta, slot)
        wait_rim(slot)
        terms = [[(part, j, beta * value) for part, j, value in found] for found in along_terms(slot, rim, bond_edge)]
        for side in range(2):
            for part, j, value in terms[side]:
                rim_send[other, 1 - side, spot(part, j)] += value
        more = n < ITERS - 3

        @pl.when(more)
        def _():
            send_rim(other)

        def put(part, r, at, value):
            pull[part, r, at : at + 1, :] += value
            field[other, part, 3 + r, PAD + at : PAD + at + 1, :] += value

        spread(terms, put)
        sum_begin(n + 2, early + (late_product(other),))

        @pl.when(more)
        def _():
            send_all(other, across)

        return alpha, beta

    one = jnp.ones((8, DEPTH), F32)
    alpha, beta = lax.fori_loop(0, ITERS - 2, cycle, (one, jnp.zeros((8, DEPTH), F32)))
    sum_middle(ITERS - 1)
    alpha, beta = damping_of(ITERS - 2, alpha, beta)
    slot = (ITERS - 2) % 2

    def last(r, carry):
        for part in range(3):
            for t in range(2):
                at = (part, r, pl.ds(8 * t, 8), slice(None))
                v, tt = v_out[at], total[at]
                v = alpha * v + beta * tt
                v_out[at] = v
                u_out[at] = u_out[at] + v
                t_out[at] = tt + alpha * rate[at] + beta * own(slot, part, r, t)
        return carry

    lax.fori_loop(0, ROWS, last, 0)
    alpha, beta = damping_of(ITERS - 1, alpha, beta)
    for t in range(2):
        a_out[8 * t : 8 * t + 8, :] = alpha
        b_out[8 * t : 8 * t + 8, :] = beta


def on_device(nx, ny, disp, vel, load, flags, mask_bits):
    block = (3, ROWS, COLS, DEPTH)
    any_spec = pl.BlockSpec(memory_space=pl.ANY)
    vmem_spec = pl.BlockSpec(memory_space=pltpu.VMEM)
    turns = ITERS
    dma = pltpu.SemaphoreType.DMA
    scratch = [
        pltpu.VMEM((SLOTS, 3, TALL, WIDE, DEPTH), F32),
        pltpu.VMEM((SLOTS, 2, 3, 2, WIDE, DEPTH), F32),
        pltpu.VMEM((SLOTS, 2, WIDE, DEPTH), F32),
        pltpu.VMEM((SLOTS, 2, 7, 24, DEPTH), F32),
        pltpu.VMEM((SLOTS, 4, 16, DEPTH), F32),
        pltpu.VMEM((SLOTS, 2, 7, 8, DEPTH), F32),
        pltpu.VMEM((SLOTS, 4, 16, DEPTH), F32),
        pltpu.VMEM((4, TALL, WIDE, DEPTH), I32),
        pltpu.VMEM((2, 4, 3, WIDE, DEPTH), I32),
        pltpu.VMEM((2, 4, 3, 24, DEPTH), I32),
        pltpu.VMEM((4, 16, DEPTH), I32),
        pltpu.VMEM((2, 4, 3, 8, DEPTH), I32),
        pltpu.VMEM((4, 16, DEPTH), I32),
        pltpu.VMEM((BONDS, ROWS * COLS, DEPTH), F32),
        pltpu.VMEM((2, len(EDGE), ROWS, DEPTH), F32),
        pltpu.VMEM((6, ROWS, COLS, DEPTH), F32),
        pltpu.VMEM((4,) + block, F32),
        pltpu.VMEM(block, F32),
        pltpu.VMEM(block[1:], I32),
        pltpu.VMEM((turns, nx, 1, DEPTH), F32),
        pltpu.VMEM((turns, ny, 1, DEPTH), F32),
        dma((7,)),
        dma((SLOTS, 10)),
        dma((SLOTS, 10)),
        dma((12,)),
        dma((12,)),
        dma((2, turns)),
        dma((2, turns)),
    ]
    u, v, total, alpha, beta = pl.pallas_call(
        functools.partial(kernel, nx, ny),
        out_shape=[pltpu.VMEM(block, F32)] * 3 + [pltpu.VMEM(block[2:], F32)] * 2,
        in_specs=[any_spec] * 5,
        out_specs=[vmem_spec] * 5,
        scratch_shapes=scratch,
        compiler_params=pltpu.CompilerParams(
            collective_id=0, has_side_effects=True, vmem_limit_bytes=60_000_000
        ),
    )(disp, vel, load, flags, mask_bits)
    v = alpha * v + beta * total
    return u + v, v


def solution(mesh):
    split = P(None, "gx", "gy", None)
    return jax.shard_map(
        functools.partial(on_device, mesh.shape["gx"], mesh.shape["gy"]),
        mesh=mesh,
        in_specs=(split, split, split, P("gx", "gy", None), split),
        out_specs=(split, split),
        check_vma=False,
    )
```

```python
import functools
import math

import jax
import jax.numpy as jnp
from jax import lax
from jax.experimental import pallas as pl
from jax.experimental.pallas import tpu as pltpu
from jax.sharding import PartitionSpec as P

ITERS = 8
MASS = 64.0
EPSILON = 1e-06
ROWS = 8
COLS = 16
DEPTH = 128
PAD = 8
WIDE = COLS + 2 * PAD
TALL = ROWS + 6
SLOTS = 4
F32 = jnp.float32
I32 = jnp.int32


def neighbour_table():
    table = []
    for across in range(-3, 4):
        for along in range(-3, 4):
            for upward in range(-3, 4):
                length = across * across + along * along + upward * upward
                if 0 < length <= 9:
                    table.append((across, along, upward))
    return table


TABLE = neighbour_table()
NUMBER = {offset: k for k, offset in enumerate(TABLE)}
BONDS = len(TABLE)


def on_axis(offset):
    return sum(1 for part in offset if part) == 1


def weight_of(offset):
    length = float(sum(part * part for part in offset))
    weight = 1.0 / (length * math.sqrt(length))
    return weight * length if on_axis(offset) else weight


def oblique(b, c):
    return [a for a in range(-2, 3) if (a, b, c) in NUMBER and not on_axis((a, b, c))]


EDGE = []
for _c in range(-2, 3):
    for _reach in (1, 2, 3):
        for _a in range(-2, 3):
            if (_a, _reach, _c) in NUMBER:
                for _j in range(_reach):
                    EDGE.append((_a, _reach, _c, _j, _reach - 1 - _j))
EDGE_AT = {entry[:4]: n for n, entry in enumerate(EDGE)}


def add(total, term):
    return term if total is None else total + term


def sub(total, term):
    return -term if total is None else total - term


def scaled(factor, value):
    if factor == 1:
        return value
    if factor == -1:
        return -value
    return float(factor) * value


def plus_scaled(total, factor, value):
    if total is None:
        return scaled(factor, value)
    if factor == 1:
        return total + value
    if factor == -1:
        return total - value
    return total + float(factor) * value


def combine(weights, totals):
    out = None
    for factor, value in zip(weights, totals):
        if factor and value is not None:
            out = plus_scaled(out, factor, value)
    return out


def accumulate_first(total, factor, value):
    if factor == 0 or value is None:
        return total
    if factor == 2:
        return value
    if factor == -2:
        return 2.0 * (total - value)
    return plus_scaled(total, factor, value)


def accumulate_square(total, factor, value):
    if factor == 0:
        return total
    if factor == 2:
        return value
    if factor == -2:
        return 4.0 * (total + value)
    return add(total, value)


def turned(value, c):
    if c == 0:
        return value
    return pltpu.roll(value, (-c) % DEPTH, 1)


def moments(terms):
    zeroth = None
    for a in sorted(terms):
        zeroth = add(zeroth, terms[a])
    first = None
    if 2 in terms:
        first = add(first, terms[2])
    if -2 in terms:
        first = sub(first, terms[-2])
    if first is not None:
        first = 2.0 * first
    if 1 in terms:
        first = add(first, terms[1])
    if -1 in terms:
        first = sub(first, terms[-1])
    return zeroth, first


def local_pass(slot, field, bond, diag, out):
    for t in range(2):
        col = PAD + 8 * t

        def coef(offset, i):
            start = i * COLS + 8 * t
            return bond[NUMBER[offset], pl.ds(start, 8), :]

        def source(part, i, b):
            return field[slot, part, 3 + i, pl.ds(col + b, 8), :]

        for c in (0, 1, -1, 2, -2, 3, -3):
            g0 = [None] * ROWS
            g1 = [None] * ROWS
            g2 = [None] * ROWS
            if c:
                for i in range(ROWS):
                    g2[i] = coef((0, 0, c), i) * source(2, i, 0)
            if c == 0:
                for i in range(ROWS):
                    for a in (1, -1, 2, -2, 3, -3):
                        if 0 <= i + a < ROWS:
                            g0[i] = add(g0[i], coef((a, 0, 0), i) * source(0, i + a, 0))
                    for b in (1, -1, 2, -2, 3, -3):
                        g1[i] = add(g1[i], coef((0, b, 0), i) * source(1, i, b))
            if abs(c) < 3:
                n0 = [None] * ROWS
                n1 = [None] * ROWS
                for b in (2, -2, 1, -1, 0):
                    reach = oblique(b, c)
                    if not reach:
                        continue
                    span = range(ROWS)
                    u0 = {i: source(0, i, b) for i in span}
                    twice = {i: 2.0 * u0[i] for i in span} if 2 in reach else None
                    u1 = {i: source(1, i, b) if b else None for i in span}
                    u2 = {i: source(2, i, b) if c else None for i in span}
                    s = {i: combine((b, c), (u1[i], u2[i])) for i in span}
                    for i in range(ROWS):
                        terms = {}
                        for a in reach:
                            if not 0 <= i + a < ROWS:
                                continue
                            near = s[i + a]
                            if abs(a) == 1:
                                near = near + u0[i + a] if a > 0 else near - u0[i + a]
                            elif a:
                                near = near + twice[i + a] if a > 0 else near - twice[i + a]
                            terms[a] = coef((a, b, c), i) * near
                        zeroth, first = moments(terms)
                        g0[i] = add(g0[i], first)
                        if c:
                            n0[i] = add(n0[i], zeroth)
                        if b == 2:
                            n1[i] = zeroth
                        elif b == -2:
                            n1[i] = 2.0 * (n1[i] - zeroth)
                        elif b:
                            n1[i] = plus_scaled(n1[i], b, zeroth)
                for i in range(ROWS):
                    g1[i] = add(g1[i], n1[i])
                    if c:
                        g2[i] = plus_scaled(g2[i], c, n0[i])
            for i in range(ROWS):
                for part, value in enumerate((g0[i], g1[i], g2[i])):
                    if c == 0:
                        if diag is not None:
                            u = [source(other, i, 0) for other in range(3)]
                            value = less_diagonal(value, diag, part, i, t, u)
                        elif value is None:
                            value = jnp.zeros((8, DEPTH), F32)
                        out[part, i, pl.ds(8 * t, 8), :] = value
                    elif value is not None:
                        out[part, i, pl.ds(8 * t, 8), :] += turned(value, c)


def less_diagonal(value, diag, part, r, t, u):
    own = None
    for other in range(3):
        pair = DIAG[min(part, other), max(part, other)]
        own = add(own, diag[pair, r, pl.ds(8 * t, 8), :] * u[other])
    return -own if value is None else value - own


DIAG = {(0, 0): 0, (0, 1): 1, (1, 1): 2, (0, 2): 3, (1, 2): 4, (2, 2): 5}


def across_pass(slot, near, far, bond, out):
    for side in range(2):
        sign = 1 if side else -1
        edge = ROWS - 1 if side else 0
        for t in range(2):
            col = PAD + 8 * t

            def coef(offset, i):
                return bond[NUMBER[offset], pl.ds((edge - sign * i) * COLS + 8 * t, 8), :]

            def source(part, layer, b):
                e = layer if side else 1 - layer
                return near[slot, side, part, e, pl.ds(col + b, 8), :]

            sums = [[None] * 3 for i in range(2)]
            third = None
            for c in (0, 1, -1, 2, -2):
                g = [[None] * 3 for i in range(2)]
                if c == 0:
                    for layer in range(2):
                        u0 = source(0, layer, 0)
                        for i in range(3):
                            a = sign * (i + layer + 1)
                            if abs(a) <= 3:
                                term = coef((a, 0, 0), i) * u0
                                if i < 2:
                                    g[i][0] = add(g[i][0], term)
                                else:
                                    third = term
                    g[0][0] = g[0][0] + coef((3 * sign, 0, 0), 0) * far[slot, side, pl.ds(col, 8), :]
                n0 = [None] * 2
                n1 = [None] * 2
                deep = [None] * 2
                for b in (2, -2, 1, -1, 0):
                    reach = oblique(b, c)
                    if not reach:
                        continue
                    zeroth = [None] * 2
                    for layer in range(max(reach)):
                        u0 = source(0, layer, b)
                        u1 = source(1, layer, b) if b else None
                        u2 = source(2, layer, b) if c else None
                        s = combine((b, c), (u1, u2))
                        for i in range(2):
                            size = i + layer + 1
                            a = sign * size
                            if a not in reach:
                                continue
                            if size == 2 and i == 1:
                                q = plus_scaled(q, sign, u0)
                            else:
                                q = plus_scaled(s, a, u0)
                            term = coef((a, b, c), i) * q
                            zeroth[i] = add(zeroth[i], term)
                            if size == 1:
                                g[i][0] = plus_scaled(g[i][0], sign, term)
                            else:
                                deep[i] = add(deep[i], term)
                    for i in range(2):
                        if zeroth[i] is None:
                            continue
                        if c:
                            n0[i] = add(n0[i], zeroth[i])
                        n1[i] = accumulate_first(n1[i], b, zeroth[i])
                for i in range(2):
                    if deep[i] is not None:
                        g[i][0] = plus_scaled(g[i][0], 2 * sign, deep[i])
                for i in range(2):
                    g[i][1] = n1[i]
                    g[i][2] = scaled(c, n0[i]) if c else None
                    for part in range(3):
                        if g[i][part] is not None:
                            sums[i][part] = add(sums[i][part], turned(g[i][part], c))
            for i in range(2):
                row = edge - sign * i
                for part in range(3):
                    out[part, row, pl.ds(8 * t, 8), :] += sums[i][part]
            out[0, edge - 2 * sign, pl.ds(8 * t, 8), :] += third


def along_terms(slot, rim, bond_edge):
    found = []
    for side in range(2):
        sign = 1 if side else -1

        def coef(a, size, c, j):
            return bond_edge[side, EDGE_AT[a, size, c, j]]

        def source(part, layer, a):
            return rim[slot, side, part * 2 + layer, pl.ds(8 + a, 8), :]

        sums = [[None] * 3 for j in range(2)]
        third = None
        for c in (0, 1, -1, 2, -2):
            g = [[None] * 3 for j in range(2)]
            if c == 0:
                for layer in range(3):
                    at = 6 if layer == 2 else 2 + layer
                    u1 = rim[slot, side, at, pl.ds(8, 8), :]
                    for j in range(3 - layer):
                        term = coef(0, layer + 1 + j, 0, j) * u1
                        if j < 2:
                            g[j][1] = add(g[j][1], term)
                        else:
                            third = term
            n0 = [None] * 2
            n1 = [None] * 2
            deep = [None] * 2
            for a in (2, -2, 1, -1, 0):
                reach = [size for size in (1, 2) if (a, size, c) in NUMBER and not on_axis((a, size, c))]
                if not reach:
                    continue
                zeroth = [None] * 2
                for layer in range(max(reach)):
                    u0 = source(0, layer, a) if a else None
                    u1 = source(1, layer, a)
                    u2 = source(2, layer, a) if c else None
                    s = combine((a, c), (u0, u2))
                    for j in range(2):
                        size = j + layer + 1
                        if size not in reach:
                            continue
                        if size == 2 and j == 1:
                            q = plus_scaled(q, sign, u1)
                        else:
                            q = plus_scaled(s, sign * size, u1)
                        term = coef(a, size, c, j) * q
                        zeroth[j] = add(zeroth[j], term)
                        if size == 1:
                            g[j][1] = plus_scaled(g[j][1], sign, term)
                        else:
                            deep[j] = add(deep[j], term)
                for j in range(2):
                    if zeroth[j] is None:
                        continue
                    if c:
                        n0[j] = add(n0[j], zeroth[j])
                    n1[j] = accumulate_first(n1[j], a, zeroth[j])
            for j in range(2):
                if deep[j] is not None:
                    g[j][1] = plus_scaled(g[j][1], 2 * sign, deep[j])
            for j in range(2):
                g[j][0] = n1[j]
                g[j][2] = scaled(c, n0[j]) if c else None
                for part in range(3):
                    if g[j][part] is not None:
                        sums[j][part] = add(sums[j][part], turned(g[j][part], c))
        found.append([(part, j, sums[j][part]) for part in range(3) for j in range(2)] + [(1, 2, third)])
    return found


def spread(found, put):
    for side in range(2):
        for part, j, value in found[side]:
            at = COLS - 1 - j if side else j
            for r in range(ROWS):
                put(part, r, at, value[r : r + 1, :])


def weight_if_intact(near, far, offset):
    k = NUMBER[offset]
    word, bit = divmod(k, 31)
    far_word, far_bit = divmod(BONDS - 1 - k, 31)
    broken = (near[word] & I32(1 << bit)) | (far(far_word) & I32(1 << far_bit))
    return jnp.where(broken == 0, F32(weight_of(offset)), F32(0.0))


def moved(own, c):
    if not c:
        return own
    lane = lax.broadcasted_iota(I32, (8, DEPTH), 1)
    outside = lane < c if c > 0 else lane >= DEPTH + c
    return [jnp.where(outside, I32(-1), pltpu.roll(word, c % DEPTH, 1)) for word in own]


def tally(sums, offset, value):
    a, b, c = offset
    if on_axis(offset):
        at = 0 if a else (2 if b else 5)
        sums[at] = add(sums[at], value)
        return
    for at, factor in enumerate((a * a, a * b, b * b, a * c, b * c, c * c)):
        if factor:
            sums[at] = plus_scaled(sums[at], factor, value)


def build_bonds(words, bond, diag):
    def row(r, carry):
        for t in range(2):
            start = pl.multiple_of(r * COLS + 8 * t, 8)
            own = [words[w, r + 3, pl.ds(PAD + 8 * t, 8), :] for w in range(4)]
            totals = [None] * 6
            for c in range(-3, 4):
                near = moved(own, c)
                sums = [None] * 6
                plain = up = twice = None
                for b in (3, -3, 2, -2, 1, -1, 0):
                    values = {}
                    for a in range(-3, 4):
                        k = NUMBER.get((a, b, c))
                        if k is None:
                            continue

                        def far(w):
                            return words[w, r + 3 + a, pl.ds(PAD + 8 * t + b, 8), :]

                        value = weight_if_intact(near, far, (a, b, c))
                        bond[k, pl.ds(start, 8), :] = value
                        if on_axis((a, b, c)):
                            tally(sums, (a, b, c), value)
                        else:
                            values[a] = value
                    if not values:
                        continue
                    zeroth, first = moments(values)
                    second = None
                    if 2 in values:
                        second = 4.0 * (values[2] + values[-2])
                    second = add(second, values[1] + values[-1])
                    sums[0] = add(sums[0], second)
                    sums[1] = accumulate_first(sums[1], b, first)
                    sums[4] = accumulate_first(sums[4], b, zeroth)
                    twice = accumulate_square(twice, b, zeroth)
                    up = add(up, first)
                    plain = add(plain, zeroth)
                sums[2] = twice if sums[2] is None else (sums[2] if twice is None else sums[2] + twice)
                if c and plain is not None:
                    sums[3] = scaled(c, up)
                    sums[5] = sums[5] + scaled(c * c, plain)
                    sums[4] = scaled(c, sums[4])
                else:
                    sums[4] = None
                for n in range(6):
                    if sums[n] is not None:
                        totals[n] = add(totals[n], turned(sums[n], c))
            for n in range(6):
                diag[n, r, pl.ds(8 * t, 8), :] = totals[n]
        return carry

    lax.fori_loop(0, ROWS, row, 0)


def build_across(words, words_near, bond, diag):
    for side in range(2):
        sign = 1 if side else -1
        edge = ROWS - 1 if side else 0
        for t in range(2):
            for i in range(3):
                r = edge - sign * i
                own = [words[w, r + 3, pl.ds(PAD + 8 * t, 8), :] for w in range(4)]
                totals = [None] * 6
                for c in range(-2, 3):
                    if i == 2 and c:
                        continue
                    near = moved(own, c)
                    sums = [None] * 6
                    for b in range(-2, 3):
                        for layer in range(3 - i):
                            offset = (sign * (i + layer + 1), b, c)
                            if offset not in NUMBER:
                                continue

                            def far(w):
                                e = layer if side else 2 - layer
                                return words_near[side, w, e, pl.ds(PAD + 8 * t + b, 8), :]

                            value = weight_if_intact(near, far, offset)
                            bond[NUMBER[offset], pl.ds(r * COLS + 8 * t, 8), :] = value
                            tally(sums, offset, value)
                    for n in range(6):
                        if sums[n] is not None:
                            totals[n] = add(totals[n], turned(sums[n], c))
                for n in range(6):
                    if totals[n] is not None:
                        diag[n, r, pl.ds(8 * t, 8), :] += totals[n]


def build_along(words_mine, words_rim, bond_edge, diag):
    for side in range(2):
        sign = 1 if side else -1
        edge = COLS - 1 if side else 0
        for j in range(3):
            own = [words_mine[1 - side, w, j] for w in range(4)]
            totals = [None] * 6
            for c in range(-2, 3):
                if j == 2 and c:
                    continue
                near = moved(own, c)
                sums = [None] * 6
                for n, (a, size, up, col, layer) in enumerate(EDGE):
                    if col != j or up != c:
                        continue
                    offset = (a, sign * size, c)

                    def far(w):
                        return words_rim[side, w, layer, pl.ds(8 + a, 8), :]

                    value = weight_if_intact(near, far, offset)
                    bond_edge[side, n] = value
                    tally(sums, offset, value)
                for n in range(6):
                    if sums[n] is not None:
                        totals[n] = add(totals[n], turned(sums[n], c))
            at = edge - sign * j
            for n in range(6):
                if totals[n] is not None:
                    for r in range(ROWS):
                        diag[n, r, at : at + 1, :] += totals[n][r : r + 1, :]


def kernel(
    nx, ny,
    disp, vel, load, flags, mask,
    u_out, v_out, t_out, a_out, b_out,
    field, near, far, rim, corner, rim_send, corner_send,
    words, words_near, words_rim, words_corner, words_rim_send, words_corner_send,
    bond, bond_edge, diag,
    pool, load_buf, flag_buf,
    ring_one, ring_two,
    in_sem, send_sem, recv_sem, word_send, word_recv, sum_send, sum_recv,
):
    total, rate, force, pull = (pool.at[n] for n in range(4))
    ax = lax.axis_index("gx")
    ay = lax.axis_index("gy")
    here = {-1: (ax > 0, ay > 0), 1: (ax < nx - 1, ay < ny - 1)}

    def exists(dx, dy):
        cond = None
        if dx:
            cond = here[dx][0]
        if dy:
            other = here[dy][1]
            cond = other if cond is None else cond & other
        return cond

    def device(dx, dy):
        return {"gx": ax + dx, "gy": ay + dy}

    sides = [(dx, dy) for dx in (-1, 0, 1) for dy in (-1, 0, 1) if dx or dy]
    diagonals = [(dx, dy) for dx, dy in sides if dx and dy]

    own_rows = pl.ds(3, ROWS)
    own_cols = pl.ds(PAD, COLS)
    loads = [
        pltpu.make_async_copy(mask, words.at[:, own_rows, own_cols], in_sem.at[0]),
        pltpu.make_async_copy(vel, field.at[1, :, own_rows, own_cols], in_sem.at[1]),
        pltpu.make_async_copy(disp, field.at[0, :, own_rows, own_cols], in_sem.at[2]),
        pltpu.make_async_copy(disp, u_out, in_sem.at[3]),
        pltpu.make_async_copy(vel, v_out, in_sem.at[4]),
        pltpu.make_async_copy(load, load_buf, in_sem.at[5]),
        pltpu.make_async_copy(flags, flag_buf, in_sem.at[6]),
    ]
    for copy in loads:
        copy.start()

    zero8 = jnp.zeros((8, DEPTH), F32)

    barrier = pltpu.get_barrier_semaphore()
    for step in range(1, nx):
        pl.semaphore_signal(barrier, inc=1, device_id={"gx": lax.rem(ax + step, nx), "gy": ay})
    for step in range(1, ny):
        pl.semaphore_signal(barrier, inc=1, device_id={"gx": ax, "gy": lax.rem(ay + step, ny)})
    for dx, dy in diagonals:
        where = {"gx": lax.rem(ax + dx + nx, nx), "gy": lax.rem(ay + dy + ny, ny)}
        pl.semaphore_signal(barrier, inc=1, device_id=where)


    inner = slice(PAD, PAD + COLS)
    pads = (slice(0, PAD), slice(PAD + COLS, WIDE))
    borders = list(range(3)) + list(range(TALL - 3, TALL))

    def broken(*shape):
        return jnp.full(shape + (DEPTH,), -1, I32)

    def clear():
        def slot_clear(slot, carry):
            for part in range(3):
                for r in borders:
                    field[slot, part, r] = jnp.zeros((WIDE, DEPTH), F32)
                for r in range(3, TALL - 3):
                    for pad in pads:
                        field[slot, part, r, pad, :] = zero8
                for side in range(2):
                    for e in range(2):
                        for pad in pads:
                            near[slot, side, part, e, pad, :] = zero8
            for side in range(2):
                for at in range(7):
                    rim[slot, side, at, 0:8, :] = zero8
                    rim[slot, side, at, 16:24, :] = zero8
            return carry

        lax.fori_loop(0, SLOTS, slot_clear, 0)
        for w in range(4):
            for r in range(TALL):
                if r in borders:
                    words[w, r] = broken(WIDE)
                else:
                    for pad in pads:
                        words[w, r, pad, :] = broken(PAD)
            for side in range(2):
                for layer in range(3):
                    for pad in pads:
                        words_near[side, w, layer, pad, :] = broken(PAD)
                    words_rim[side, w, layer, 0:8, :] = broken(8)
                    words_rim[side, w, layer, 16:24, :] = broken(8)
        for side in range(2):
            @pl.when(ax == (nx - 1 if side else 0))
            def _():
                for slot in range(SLOTS):
                    far[slot, side, inner, :] = jnp.zeros((COLS, DEPTH), F32)
                    for part in range(3):
                        for e in range(2):
                            near[slot, side, part, e, inner, :] = jnp.zeros((COLS, DEPTH), F32)
                for w in range(4):
                    for layer in range(3):
                        words_near[side, w, layer, inner, :] = broken(COLS)

            @pl.when(ay == (ny - 1 if side else 0))
            def _():
                for slot in range(SLOTS):
                    for at in range(7):
                        rim[slot, side, at, 8:16, :] = zero8
                for w in range(4):
                    for layer in range(3):
                        words_rim[side, w, layer, 8:16, :] = broken(8)

    def edge_rows(dx):
        return (0, 2) if dx < 0 else (ROWS - 2, ROWS - 3)

    def halo_copies(slot, dx, dy):
        into = {-1: 1, 1: 0}
        if dx and dy:
            n = into[dx] * 2 + into[dy]
            return [(corner_send.at[slot, n], corner.at[slot, n], 6 + n)]
        if dx:
            first, third = edge_rows(dx)
            side = into[dx]
            return [
                (
                    field.at[slot, :, pl.ds(3 + first, 2), own_cols],
                    near.at[slot, side, :, :, own_cols],
                    side,
                ),
                (field.at[slot, 0, 3 + third, own_cols], far.at[slot, side, own_cols], 2 + side),
            ]
        side = into[dy]
        return [(rim_send.at[slot, side], rim.at[slot, side, :, pl.ds(8, 8)], 4 + side)]

    def spot(part, layer):
        return 6 if layer == 2 else part * 2 + layer

    def pack_rim(slot):
        for side in range(2):
            for part in range(3):
                for layer in range(3 if part == 1 else 2):
                    col = PAD + (layer if side else COLS - 1 - layer)
                    for r in range(ROWS):
                        rim_send[slot, side, spot(part, layer), r : r + 1, :] = field[
                            slot, part, 3 + r, col : col + 1, :
                        ]

    def ends(dx):
        return slice(0, 2) if dx < 0 else slice(ROWS - 2, ROWS)

    def beyond(dx):
        return slice(6, 8) if dx < 0 else slice(16, 18)

    def copy_of(slot, dx, dy, src, dst, n):
        return pltpu.make_async_remote_copy(
            src_ref=src, dst_ref=dst, send_sem=send_sem.at[slot, n], recv_sem=recv_sem.at[slot, n],
            device_id=device(dx, dy),
        )

    along = [(0, -1), (0, 1)]
    across = [(-1, 0), (1, 0)]

    def send_all(slot, which):
        for dx, dy in which:
            @pl.when(exists(dx, dy))
            def _():
                for src, dst, n in halo_copies(slot, dx, dy):
                    copy_of(slot, dx, dy, src, dst, n).start()

    def send_rim(slot):
        send_all(slot, along)
        for dx, dy in diagonals:
            n = (1 if dx < 0 else 0) * 2 + (1 if dy < 0 else 0)
            for at in range(6):
                corner_send[slot, n, 2 * at : 2 * at + 2, :] = rim_send[slot, 1 if dy < 0 else 0, at, ends(dx), :]
        send_all(slot, diagonals)

    def halo_send(slot):
        pack_rim(slot)
        send_rim(slot)
        send_all(slot, across)

    def wait_all(slot, which):
        for dx, dy in which:
            @pl.when(exists(dx, dy))
            def _():
                for src, dst, n in halo_copies(slot, dx, dy):
                    copy_of(slot, dx, dy, src, dst, n).wait_send()
                for src, dst, n in halo_copies(slot, -dx, -dy):
                    copy_of(slot, dx, dy, src, dst, n).wait_recv()

    def wait_rim(slot):
        wait_all(slot, along + diagonals)
        for dx, dy in diagonals:
            sx, sy = (1 if dx > 0 else 0), (1 if dy > 0 else 0)

            @pl.when(exists(dx, dy))
            def _():
                for at in range(6):
                    rim[slot, sy, at, beyond(dx), :] = corner[slot, sx * 2 + sy, 2 * at : 2 * at + 2, :]

    def word_copies(dx, dy):
        into = {-1: 1, 1: 0}
        if dx and dy:
            n = into[dx] * 2 + into[dy]
            return [(words_corner_send.at[n], words_corner.at[n], 4 + n)]
        if dx:
            side = into[dx]
            first, third = edge_rows(dx)
            two, one = (pl.ds(0, 2), 2) if side else (pl.ds(1, 2), 0)
            w = third_word((3, 0, 0), side)
            return [
                (words.at[:, pl.ds(3 + first, 2), own_cols], words_near.at[side, :, two, own_cols], side),
                (words.at[w, 3 + third, own_cols], words_near.at[side, w, one, own_cols], 8 + side),
            ]
        side = into[dy]
        w = third_word((0, 3, 0), side)
        two = pl.ds(0, 2)
        return [
            (words_rim_send.at[side, :, two], words_rim.at[side, :, two, pl.ds(8, 8)], 2 + side),
            (words_rim_send.at[side, w, 2], words_rim.at[side, w, 2, pl.ds(8, 8)], 10 + side),
        ]

    def third_word(offset, side):
        if not side:
            offset = tuple(-part for part in offset)
        return (BONDS - 1 - NUMBER[offset]) // 31

    def word_copy(dx, dy, src, dst, n):
        return pltpu.make_async_remote_copy(
            src_ref=src, dst_ref=dst, send_sem=word_send.at[n], recv_sem=word_recv.at[n], device_id=device(dx, dy),
        )

    loads[0].wait()
    for side in range(2):
        for w in range(4):
            for layer in range(3):
                col = PAD + (layer if side else COLS - 1 - layer)
                for r in range(ROWS):
                    words_rim_send[side, w, layer, r : r + 1, :] = words[w, 3 + r, col : col + 1, :]
    for dx, dy in diagonals:
        n = (1 if dx < 0 else 0) * 2 + (1 if dy < 0 else 0)
        for w in range(4):
            for layer in range(2):
                at = (w * 2 + layer) * 2
                words_corner_send[n, at : at + 2, :] = words_rim_send[1 if dy < 0 else 0, w, layer, ends(dx), :]
    clear()
    pl.semaphore_wait(barrier, nx + ny + 2)
    for dx, dy in sides:
        @pl.when(exists(dx, dy))
        def _():
            for src, dst, n in word_copies(dx, dy):
                word_copy(dx, dy, src, dst, n).start()
    loads[2].wait()
    halo_send(0)

    build_bonds(words, bond, diag)
    loads[1].wait()
    halo_send(1)
    def words_wait(which):
        for dx, dy in which:
            @pl.when(exists(dx, dy))
            def _():
                for src, dst, n in word_copies(dx, dy):
                    word_copy(dx, dy, src, dst, n).wait_send()
                for src, dst, n in word_copies(-dx, -dy):
                    word_copy(dx, dy, src, dst, n).wait_recv()

    def words_across():
        words_wait(across)
        build_across(words, words_near, bond, diag)

    def words_along():
        words_wait(along + diagonals)
        for dx, dy in diagonals:
            sx, sy = (1 if dx > 0 else 0), (1 if dy > 0 else 0)

            @pl.when(exists(dx, dy))
            def _():
                for w in range(4):
                    for layer in range(2):
                        at = (w * 2 + layer) * 2
                        words_rim[sy, w, layer, beyond(dx), :] = words_corner[sx * 2 + sy, at : at + 2, :]

        build_along(words_rim_send, words_rim, bond_edge, diag)

    def sum_copy(src, dst, which, turn, where):
        return pltpu.make_async_remote_copy(
            src_ref=src, dst_ref=dst, send_sem=sum_send.at[which, turn], recv_sem=sum_recv.at[which, turn],
            device_id=where,
        )

    def sum_begin(turn, rows):
        slab = jnp.concatenate([jnp.sum(row, axis=0, keepdims=True) for row in rows] + [jnp.zeros((2, DEPTH), F32)], axis=0)
        each = jnp.broadcast_to(jnp.sum(slab, axis=1, keepdims=True), (8, DEPTH))
        mine = lax.broadcasted_iota(I32, (8, DEPTH), 0) == lax.broadcasted_iota(I32, (8, DEPTH), 1)
        ring_one[turn, ax] = jnp.sum(jnp.where(mine, each, 0.0), axis=0, keepdims=True)
        for step in range(1, nx):
            sum_copy(
                ring_one.at[turn, ax], ring_one.at[turn, ax], 0, turn, {"gx": lax.rem(ax + step, nx), "gy": ay}
            ).start()

    def sum_middle(turn):
        some = ring_one.at[turn, pl.ds(0, nx - 1)]
        copy = sum_copy(some, some, 0, turn, {"gx": ax, "gy": ay})
        copy.wait_recv()
        copy.wait_send()
        ring_two[turn, ay] = jnp.sum(ring_one[turn], axis=0)
        for step in range(1, ny):
            sum_copy(
                ring_two.at[turn, ay], ring_two.at[turn, ay], 1, turn, {"gx": ax, "gy": lax.rem(ay + step, ny)}
            ).start()

    def sum_end(turn):
        some = ring_two.at[turn, pl.ds(0, ny - 1)]
        copy = sum_copy(some, some, 1, turn, {"gx": ax, "gy": ay})
        copy.wait_recv()
        copy.wait_send()
        row = jnp.sum(ring_two[turn], axis=0)
        return [jnp.broadcast_to(row[:, n : n + 1], (8, DEPTH)) for n in range(6)]

    count = 3.0 * ROWS * nx * COLS * ny * DEPTH

    def damping_of(turn, alpha, beta):
        g0, g1, g2, h0, h1, h2 = sum_end(turn)
        kinetic = alpha * alpha * g0 + 2.0 * alpha * beta * g1 + beta * beta * g2
        rayleigh = -(alpha * alpha * h0 + 2.0 * alpha * beta * h1 + beta * beta * h2)
        rayleigh = jnp.maximum(rayleigh, 0.0)
        damping = 2.0 * jnp.sqrt((rayleigh / count) / (MASS * (kinetic / count + EPSILON)))
        return (2.0 - damping) / (2.0 + damping), 2.0 / (MASS * (2.0 + damping))

    def own(ref_slot, part, r, t):
        return field[ref_slot, part, 3 + r, pl.ds(PAD + 8 * t, 8), :]

    vregs = [(part, r, t) for part in range(3) for r in range(ROWS) for t in range(2)]

    def tally_pair(acc, v, t, w):
        return (acc[0] + v * v, acc[1] + v * t, acc[2] + t * t, acc[3] + v * w, acc[4] + t * w)

    def early_products():
        def body(r, acc):
            for part in range(3):
                for t in range(2):
                    at = (part, r, pl.ds(8 * t, 8), slice(None))
                    acc = tally_pair(acc, v_out[at], total[at], rate[at])
            return acc

        return lax.fori_loop(0, ROWS, body, (zero8,) * 5)

    def late_product(slot):
        def body(r, acc):
            acc = list(acc)
            for part in range(3):
                for t in range(2):
                    acc[t] = acc[t] + total[part, r, pl.ds(8 * t, 8), :] * own(slot, part, r, t)
            return tuple(acc)

        acc = lax.fori_loop(0, ROWS, body, (zero8,) * 2)
        return acc[0] + acc[1]

    def rest(slot, out, meanwhile):
        wait_all(slot, across)
        across_pass(slot, near, far, bond, out)
        meanwhile()
        wait_rim(slot)

        def put(part, r, at, value):
            out[part, r, at : at + 1, :] += value

        spread(along_terms(slot, rim, bond_edge), put)

    for copy in loads[3:]:
        copy.wait()

    def begin(n, carry):
        out = pool.at[n]
        local_pass(n, field, bond, None, out)

        @pl.when(n == 0)
        def _():
            words_across()

        def meanwhile():
            @pl.when(n == 0)
            def _():
                words_along()

        rest(n, out, meanwhile)
        loaded = lax.div(3 - n, 3).astype(F32)
        to = lax.rem(n + 2, 4)

        def put(r, carry):
            for t in range(2):
                at = (r, pl.ds(8 * t, 8), slice(None))
                active = loaded * flag_buf[at].astype(F32)
                u = [own(n, part, r, t) for part in range(3)]
                for part in range(3):
                    value = less_diagonal(out[(part,) + at], diag, part, r, t, u)
                    value = value + active * load_buf[(part,) + at]
                    out[(part,) + at] = value
                    field[to, part, 3 + r, pl.ds(PAD + 8 * t, 8), :] = value
            return carry

        lax.fori_loop(0, ROWS, put, 0)

        @pl.when(n < 3)
        def _():
            halo_send(to)

        @pl.when(n == 1)
        def _():
            sum_begin(0, early_products() + (zero8,))

        @pl.when(n == 2)
        def _():
            sum_middle(0)
            sum_begin(1, early_products() + (late_product(0),))

        return carry

    lax.fori_loop(0, 4, begin, 0)

    def advance(alpha, beta, slot):
        def body(r, acc):
            for part in range(3):
                for t in range(2):
                    at = (part, r, pl.ds(8 * t, 8), slice(None))
                    v, tt, w, y = v_out[at], total[at], rate[at], own(slot, part, r, t)
                    v = alpha * v + beta * tt
                    w = alpha * w + beta * y
                    tt = tt + w
                    v_out[at] = v
                    u_out[at] = u_out[at] + v
                    rate[at] = w
                    total[at] = tt
                    acc = tally_pair(acc, v, tt, w)
            return acc

        return lax.fori_loop(0, ROWS, body, (zero8,) * 5)

    def cycle(n, carry):
        alpha, beta = carry
        slot = lax.rem(n, 2)
        other = 1 - slot
        local_pass(slot, field, bond, diag, force)
        wait_all(slot, across)
        across_pass(slot, near, far, bond, force)
        sum_middle(n + 1)
        alpha, beta = damping_of(n, alpha, beta)

        def body(r, carry):
            for part in range(3):
                for t in range(2):
                    at = (part, r, pl.ds(8 * t, 8), slice(None))
                    x = alpha * pull[at] + beta * force[at]
                    pull[at] = x
                    field[other, part, 3 + r, pl.ds(PAD + 8 * t, 8), :] = own(slot, part, r, t) + x
            return carry

        lax.fori_loop(0, ROWS, body, 0)
        pack_rim(other)
        early = advance(alpha, beta, slot)
        wait_rim(slot)
        terms = [[(part, j, beta * value) for part, j, value in found] for found in along_terms(slot, rim, bond_edge)]
        for side in range(2):
            for part, j, value in terms[side]:
                rim_send[other, 1 - side, spot(part, j)] += value
        more = n < ITERS - 3

        @pl.when(more)
        def _():
            send_rim(other)

        def put(part, r, at, value):
            pull[part, r, at : at + 1, :] += value
            field[other, part, 3 + r, PAD + at : PAD + at + 1, :] += value

        spread(terms, put)
        sum_begin(n + 2, early + (late_product(other),))

        @pl.when(more)
        def _():
            send_all(other, across)

        return alpha, beta

    one = jnp.ones((8, DEPTH), F32)
    alpha, beta = lax.fori_loop(0, ITERS - 2, cycle, (one, jnp.zeros((8, DEPTH), F32)))
    sum_middle(ITERS - 1)
    alpha, beta = damping_of(ITERS - 2, alpha, beta)
    slot = (ITERS - 2) % 2

    def last(r, carry):
        for part in range(3):
            for t in range(2):
                at = (part, r, pl.ds(8 * t, 8), slice(None))
                v, tt = v_out[at], total[at]
                v = alpha * v + beta * tt
                v_out[at] = v
                u_out[at] = u_out[at] + v
                t_out[at] = tt + alpha * rate[at] + beta * own(slot, part, r, t)
        return carry

    lax.fori_loop(0, ROWS, last, 0)
    alpha, beta = damping_of(ITERS - 1, alpha, beta)
    for t in range(2):
        a_out[8 * t : 8 * t + 8, :] = alpha
        b_out[8 * t : 8 * t + 8, :] = beta


def on_device(nx, ny, disp, vel, load, flags, mask_bits):
    block = (3, ROWS, COLS, DEPTH)
    any_spec = pl.BlockSpec(memory_space=pl.ANY)
    vmem_spec = pl.BlockSpec(memory_space=pltpu.VMEM)
    turns = ITERS
    dma = pltpu.SemaphoreType.DMA
    scratch = [
        pltpu.VMEM((SLOTS, 3, TALL, WIDE, DEPTH), F32),
        pltpu.VMEM((SLOTS, 2, 3, 2, WIDE, DEPTH), F32),
        pltpu.VMEM((SLOTS, 2, WIDE, DEPTH), F32),
        pltpu.VMEM((SLOTS, 2, 7, 24, DEPTH), F32),
        pltpu.VMEM((SLOTS, 4, 16, DEPTH), F32),
        pltpu.VMEM((SLOTS, 2, 7, 8, DEPTH), F32),
        pltpu.VMEM((SLOTS, 4, 16, DEPTH), F32),
        pltpu.VMEM((4, TALL, WIDE, DEPTH), I32),
        pltpu.VMEM((2, 4, 3, WIDE, DEPTH), I32),
        pltpu.VMEM((2, 4, 3, 24, DEPTH), I32),
        pltpu.VMEM((4, 16, DEPTH), I32),
        pltpu.VMEM((2, 4, 3, 8, DEPTH), I32),
        pltpu.VMEM((4, 16, DEPTH), I32),
        pltpu.VMEM((BONDS, ROWS * COLS, DEPTH), F32),
        pltpu.VMEM((2, len(EDGE), ROWS, DEPTH), F32),
        pltpu.VMEM((6, ROWS, COLS, DEPTH), F32),
        pltpu.VMEM((4,) + block, F32),
        pltpu.VMEM(block, F32),
        pltpu.VMEM(block[1:], I32),
        pltpu.VMEM((turns, nx, 1, DEPTH), F32),
        pltpu.VMEM((turns, ny, 1, DEPTH), F32),
        dma((7,)),
        dma((SLOTS, 10)),
        dma((SLOTS, 10)),
        dma((12,)),
        dma((12,)),
        dma((2, turns)),
        dma((2, turns)),
    ]
    u, v, total, alpha, beta = pl.pallas_call(
        functools.partial(kernel, nx, ny),
        out_shape=[pltpu.VMEM(block, F32)] * 3 + [pltpu.VMEM(block[2:], F32)] * 2,
        in_specs=[any_spec] * 5,
        out_specs=[vmem_spec] * 5,
        scratch_shapes=scratch,
        compiler_params=pltpu.CompilerParams(
            collective_id=0, has_side_effects=True, vmem_limit_bytes=60_000_000
        ),
    )(disp, vel, load, flags, mask_bits)
    v = alpha * v + beta * total
    return u + v, v


def solution(mesh):
    split = P(None, "gx", "gy", None)
    return jax.shard_map(
        functools.partial(on_device, mesh.shape["gx"], mesh.shape["gy"]),
        mesh=mesh,
        in_specs=(split, split, split, P("gx", "gy", None), split),
        out_specs=(split, split),
        check_vma=False,
    )
```

```python
import functools
import math

import jax
import jax.numpy as jnp
from jax import lax
from jax.experimental import pallas as pl
from jax.experimental.pallas import tpu as pltpu
from jax.sharding import PartitionSpec as P

ITERS = 8
MASS = 64.0
EPSILON = 1e-06
ROWS = 8
COLS = 16
DEPTH = 128
PAD = 8
WIDE = COLS + 2 * PAD
TALL = ROWS + 6
SLOTS = 4
F32 = jnp.float32
I32 = jnp.int32


def neighbour_table():
    table = []
    for across in range(-3, 4):
        for along in range(-3, 4):
            for upward in range(-3, 4):
                length = across * across + along * along + upward * upward
                if 0 < length <= 9:
                    table.append((across, along, upward))
    return table


TABLE = neighbour_table()
NUMBER = {offset: k for k, offset in enumerate(TABLE)}
BONDS = len(TABLE)


def on_axis(offset):
    return sum(1 for part in offset if part) == 1


def weight_of(offset):
    length = float(sum(part * part for part in offset))
    weight = 1.0 / (length * math.sqrt(length))
    return weight * length if on_axis(offset) else weight


def oblique(b, c):
    return [a for a in range(-2, 3) if (a, b, c) in NUMBER and not on_axis((a, b, c))]


EDGE = []
for _c in range(-2, 3):
    for _reach in (1, 2, 3):
        for _a in range(-2, 3):
            if (_a, _reach, _c) in NUMBER:
                for _j in range(_reach):
                    EDGE.append((_a, _reach, _c, _j, _reach - 1 - _j))
EDGE_AT = {entry[:4]: n for n, entry in enumerate(EDGE)}


def add(total, term):
    return term if total is None else total + term


def sub(total, term):
    return -term if total is None else total - term


def scaled(factor, value):
    if factor == 1:
        return value
    if factor == -1:
        return -value
    return float(factor) * value


def plus_scaled(total, factor, value):
    if total is None:
        return scaled(factor, value)
    if factor == 1:
        return total + value
    if factor == -1:
        return total - value
    return total + float(factor) * value


def combine(weights, totals):
    out = None
    for factor, value in zip(weights, totals):
        if factor and value is not None:
            out = plus_scaled(out, factor, value)
    return out


def accumulate_first(total, factor, value):
    if factor == 0 or value is None:
        return total
    if factor == 2:
        return value
    if factor == -2:
        return 2.0 * (total - value)
    return plus_scaled(total, factor, value)


def accumulate_square(total, factor, value):
    if factor == 0:
        return total
    if factor == 2:
        return value
    if factor == -2:
        return 4.0 * (total + value)
    return add(total, value)


def turned(value, c):
    if c == 0:
        return value
    return pltpu.roll(value, (-c) % DEPTH, 1)


def moments(terms):
    zeroth = None
    for a in sorted(terms):
        zeroth = add(zeroth, terms[a])
    first = None
    if 2 in terms:
        first = add(first, terms[2])
    if -2 in terms:
        first = sub(first, terms[-2])
    if first is not None:
        first = 2.0 * first
    if 1 in terms:
        first = add(first, terms[1])
    if -1 in terms:
        first = sub(first, terms[-1])
    return zeroth, first


def local_pass(slot, field, bond, diag, out):
    for t in range(2):
        col = PAD + 8 * t

        def coef(offset, i):
            start = i * COLS + 8 * t
            return bond[NUMBER[offset], pl.ds(start, 8), :]

        def source(part, i, b):
            return field[slot, part, 3 + i, pl.ds(col + b, 8), :]

        for c in (0, 1, -1, 2, -2, 3, -3):
            g0 = [None] * ROWS
            g1 = [None] * ROWS
            g2 = [None] * ROWS
            if c:
                for i in range(ROWS):
                    g2[i] = coef((0, 0, c), i) * source(2, i, 0)
            if c == 0:
                for i in range(ROWS):
                    for a in (1, -1, 2, -2, 3, -3):
                        if 0 <= i + a < ROWS:
                            g0[i] = add(g0[i], coef((a, 0, 0), i) * source(0, i + a, 0))
                    for b in (1, -1, 2, -2, 3, -3):
                        g1[i] = add(g1[i], coef((0, b, 0), i) * source(1, i, b))
            if abs(c) < 3:
                n0 = [None] * ROWS
                n1 = [None] * ROWS
                for b in (2, -2, 1, -1, 0):
                    reach = oblique(b, c)
                    if not reach:
                        continue
                    span = range(ROWS)
                    u0 = {i: source(0, i, b) for i in span}
                    twice = {i: 2.0 * u0[i] for i in span} if 2 in reach else None
                    u1 = {i: source(1, i, b) if b else None for i in span}
                    u2 = {i: source(2, i, b) if c else None for i in span}
                    s = {i: combine((b, c), (u1[i], u2[i])) for i in span}
                    for i in range(ROWS):
                        terms = {}
                        for a in reach:
                            if not 0 <= i + a < ROWS:
                                continue
                            near = s[i + a]
                            if abs(a) == 1:
                                near = near + u0[i + a] if a > 0 else near - u0[i + a]
                            elif a:
                                near = near + twice[i + a] if a > 0 else near - twice[i + a]
                            terms[a] = coef((a, b, c), i) * near
                        zeroth, first = moments(terms)
                        g0[i] = add(g0[i], first)
                        if c:
                            n0[i] = add(n0[i], zeroth)
                        if b == 2:
                            n1[i] = zeroth
                        elif b == -2:
                            n1[i] = 2.0 * (n1[i] - zeroth)
                        elif b:
                            n1[i] = plus_scaled(n1[i], b, zeroth)
                for i in range(ROWS):
                    g1[i] = add(g1[i], n1[i])
                    if c:
                        g2[i] = plus_scaled(g2[i], c, n0[i])
            for i in range(ROWS):
                for part, value in enumerate((g0[i], g1[i], g2[i])):
                    if c == 0:
                        if diag is not None:
                            u = [source(other, i, 0) for other in range(3)]
                            value = less_diagonal(value, diag, part, i, t, u)
                        elif value is None:
                            value = jnp.zeros((8, DEPTH), F32)
                        out[part, i, pl.ds(8 * t, 8), :] = value
                    elif value is not None:
                        out[part, i, pl.ds(8 * t, 8), :] += turned(value, c)


def less_diagonal(value, diag, part, r, t, u):
    own = None
    for other in range(3):
        pair = DIAG[min(part, other), max(part, other)]
        own = add(own, diag[pair, r, pl.ds(8 * t, 8), :] * u[other])
    return -own if value is None else value - own


DIAG = {(0, 0): 0, (0, 1): 1, (1, 1): 2, (0, 2): 3, (1, 2): 4, (2, 2): 5}


def across_pass(slot, near, far, bond, out):
    for side in range(2):
        sign = 1 if side else -1
        edge = ROWS - 1 if side else 0
        for t in range(2):
            col = PAD + 8 * t

            def coef(offset, i):
                return bond[NUMBER[offset], pl.ds((edge - sign * i) * COLS + 8 * t, 8), :]

            def source(part, layer, b):
                e = layer if side else 1 - layer
                return near[slot, side, part, e, pl.ds(col + b, 8), :]

            sums = [[None] * 3 for i in range(2)]
            third = None
            for c in (0, 1, -1, 2, -2):
                g = [[None] * 3 for i in range(2)]
                if c == 0:
                    for layer in range(2):
                        u0 = source(0, layer, 0)
                        for i in range(3):
                            a = sign * (i + layer + 1)
                            if abs(a) <= 3:
                                term = coef((a, 0, 0), i) * u0
                                if i < 2:
                                    g[i][0] = add(g[i][0], term)
                                else:
                                    third = term
                    g[0][0] = g[0][0] + coef((3 * sign, 0, 0), 0) * far[slot, side, pl.ds(col, 8), :]
                n0 = [None] * 2
                n1 = [None] * 2
                deep = [None] * 2
                for b in (2, -2, 1, -1, 0):
                    reach = oblique(b, c)
                    if not reach:
                        continue
                    zeroth = [None] * 2
                    for layer in range(max(reach)):
                        u0 = source(0, layer, b)
                        u1 = source(1, layer, b) if b else None
                        u2 = source(2, layer, b) if c else None
                        s = combine((b, c), (u1, u2))
                        for i in range(2):
                            size = i + layer + 1
                            a = sign * size
                            if a not in reach:
                                continue
                            if size == 2 and i == 1:
                                q = plus_scaled(q, sign, u0)
                            else:
                                q = plus_scaled(s, a, u0)
                            term = coef((a, b, c), i) * q
                            zeroth[i] = add(zeroth[i], term)
                            if size == 1:
                                g[i][0] = plus_scaled(g[i][0], sign, term)
                            else:
                                deep[i] = add(deep[i], term)
                    for i in range(2):
                        if zeroth[i] is None:
                            continue
                        if c:
                            n0[i] = add(n0[i], zeroth[i])
                        n1[i] = accumulate_first(n1[i], b, zeroth[i])
                for i in range(2):
                    if deep[i] is not None:
                        g[i][0] = plus_scaled(g[i][0], 2 * sign, deep[i])
                for i in range(2):
                    g[i][1] = n1[i]
                    g[i][2] = scaled(c, n0[i]) if c else None
                    for part in range(3):
                        if g[i][part] is not None:
                            sums[i][part] = add(sums[i][part], turned(g[i][part], c))
            for i in range(2):
                row = edge - sign * i
                for part in range(3):
                    out[part, row, pl.ds(8 * t, 8), :] += sums[i][part]
            out[0, edge - 2 * sign, pl.ds(8 * t, 8), :] += third


def along_terms(slot, rim, bond_edge):
    found = []
    for side in range(2):
        sign = 1 if side else -1

        def coef(a, size, c, j):
            return bond_edge[side, EDGE_AT[a, size, c, j]]

        def source(part, layer, a):
            return rim[slot, side, part * 2 + layer, pl.ds(8 + a, 8), :]

        sums = [[None] * 3 for j in range(2)]
        third = None
        for c in (0, 1, -1, 2, -2):
            g = [[None] * 3 for j in range(2)]
            if c == 0:
                for layer in range(3):
                    at = 6 if layer == 2 else 2 + layer
                    u1 = rim[slot, side, at, pl.ds(8, 8), :]
                    for j in range(3 - layer):
                        term = coef(0, layer + 1 + j, 0, j) * u1
                        if j < 2:
                            g[j][1] = add(g[j][1], term)
                        else:
                            third = term
            n0 = [None] * 2
            n1 = [None] * 2
            deep = [None] * 2
            for a in (2, -2, 1, -1, 0):
                reach = [size for size in (1, 2) if (a, size, c) in NUMBER and not on_axis((a, size, c))]
                if not reach:
                    continue
                zeroth = [None] * 2
                for layer in range(max(reach)):
                    u0 = source(0, layer, a) if a else None
                    u1 = source(1, layer, a)
                    u2 = source(2, layer, a) if c else None
                    s = combine((a, c), (u0, u2))
                    for j in range(2):
                        size = j + layer + 1
                        if size not in reach:
                            continue
                        if size == 2 and j == 1:
                            q = plus_scaled(q, sign, u1)
                        else:
                            q = plus_scaled(s, sign * size, u1)
                        term = coef(a, size, c, j) * q
                        zeroth[j] = add(zeroth[j], term)
                        if size == 1:
                            g[j][1] = plus_scaled(g[j][1], sign, term)
                        else:
                            deep[j] = add(deep[j], term)
                for j in range(2):
                    if zeroth[j] is None:
                        continue
                    if c:
                        n0[j] = add(n0[j], zeroth[j])
                    n1[j] = accumulate_first(n1[j], a, zeroth[j])
            for j in range(2):
                if deep[j] is not None:
                    g[j][1] = plus_scaled(g[j][1], 2 * sign, deep[j])
            for j in range(2):
                g[j][0] = n1[j]
                g[j][2] = scaled(c, n0[j]) if c else None
                for part in range(3):
                    if g[j][part] is not None:
                        sums[j][part] = add(sums[j][part], turned(g[j][part], c))
        found.append([(part, j, sums[j][part]) for part in range(3) for j in range(2)] + [(1, 2, third)])
    return found


def spread(found, put):
    for side in range(2):
        for part, j, value in found[side]:
            at = COLS - 1 - j if side else j
            for r in range(ROWS):
                put(part, r, at, value[r : r + 1, :])


def weight_if_intact(near, far, offset):
    k = NUMBER[offset]
    word, bit = divmod(k, 31)
    far_word, far_bit = divmod(BONDS - 1 - k, 31)
    broken = (near[word] & I32(1 << bit)) | (far(far_word) & I32(1 << far_bit))
    return jnp.where(broken == 0, F32(weight_of(offset)), F32(0.0))


def moved(own, c):
    if not c:
        return own
    lane = lax.broadcasted_iota(I32, (8, DEPTH), 1)
    outside = lane < c if c > 0 else lane >= DEPTH + c
    return [jnp.where(outside, I32(-1), pltpu.roll(word, c % DEPTH, 1)) for word in own]


def tally(sums, offset, value):
    a, b, c = offset
    if on_axis(offset):
        at = 0 if a else (2 if b else 5)
        sums[at] = add(sums[at], value)
        return
    for at, factor in enumerate((a * a, a * b, b * b, a * c, b * c, c * c)):
        if factor:
            sums[at] = plus_scaled(sums[at], factor, value)


def build_bonds(words, bond, diag):
    def row(r, carry):
        for t in range(2):
            start = pl.multiple_of(r * COLS + 8 * t, 8)
            own = [words[w, r + 3, pl.ds(PAD + 8 * t, 8), :] for w in range(4)]
            totals = [None] * 6
            for c in range(-3, 4):
                near = moved(own, c)
                sums = [None] * 6
                plain = up = twice = None
                for b in (3, -3, 2, -2, 1, -1, 0):
                    values = {}
                    for a in range(-3, 4):
                        k = NUMBER.get((a, b, c))
                        if k is None:
                            continue

                        def far(w):
                            return words[w, r + 3 + a, pl.ds(PAD + 8 * t + b, 8), :]

                        value = weight_if_intact(near, far, (a, b, c))
                        bond[k, pl.ds(start, 8), :] = value
                        if on_axis((a, b, c)):
                            tally(sums, (a, b, c), value)
                        else:
                            values[a] = value
                    if not values:
                        continue
                    zeroth, first = moments(values)
                    second = None
                    if 2 in values:
                        second = 4.0 * (values[2] + values[-2])
                    second = add(second, values[1] + values[-1])
                    sums[0] = add(sums[0], second)
                    sums[1] = accumulate_first(sums[1], b, first)
                    sums[4] = accumulate_first(sums[4], b, zeroth)
                    twice = accumulate_square(twice, b, zeroth)
                    up = add(up, first)
                    plain = add(plain, zeroth)
                sums[2] = twice if sums[2] is None else (sums[2] if twice is None else sums[2] + twice)
                if c and plain is not None:
                    sums[3] = scaled(c, up)
                    sums[5] = sums[5] + scaled(c * c, plain)
                    sums[4] = scaled(c, sums[4])
                else:
                    sums[4] = None
                for n in range(6):
                    if sums[n] is not None:
                        totals[n] = add(totals[n], turned(sums[n], c))
            for n in range(6):
                diag[n, r, pl.ds(8 * t, 8), :] = totals[n]
        return carry

    lax.fori_loop(0, ROWS, row, 0)


def build_across(words, words_near, bond, diag):
    for side in range(2):
        sign = 1 if side else -1
        edge = ROWS - 1 if side else 0
        for t in range(2):
            for i in range(3):
                r = edge - sign * i
                own = [words[w, r + 3, pl.ds(PAD + 8 * t, 8), :] for w in range(4)]
                totals = [None] * 6
                for c in range(-2, 3):
                    if i == 2 and c:
                        continue
                    near = moved(own, c)
                    sums = [None] * 6
                    for b in range(-2, 3):
                        for layer in range(3 - i):
                            offset = (sign * (i + layer + 1), b, c)
                            if offset not in NUMBER:
                                continue

                            def far(w):
                                e = layer if side else 2 - layer
                                return words_near[side, w, e, pl.ds(PAD + 8 * t + b, 8), :]

                            value = weight_if_intact(near, far, offset)
                            bond[NUMBER[offset], pl.ds(r * COLS + 8 * t, 8), :] = value
                            tally(sums, offset, value)
                    for n in range(6):
                        if sums[n] is not None:
                            totals[n] = add(totals[n], turned(sums[n], c))
                for n in range(6):
                    if totals[n] is not None:
                        diag[n, r, pl.ds(8 * t, 8), :] += totals[n]


def build_along(words_mine, words_rim, bond_edge, diag):
    for side in range(2):
        sign = 1 if side else -1
        edge = COLS - 1 if side else 0
        for j in range(3):
            own = [words_mine[1 - side, w, j] for w in range(4)]
            totals = [None] * 6
            for c in range(-2, 3):
                if j == 2 and c:
                    continue
                near = moved(own, c)
                sums = [None] * 6
                for n, (a, size, up, col, layer) in enumerate(EDGE):
                    if col != j or up != c:
                        continue
                    offset = (a, sign * size, c)

                    def far(w):
                        return words_rim[side, w, layer, pl.ds(8 + a, 8), :]

                    value = weight_if_intact(near, far, offset)
                    bond_edge[side, n] = value
                    tally(sums, offset, value)
                for n in range(6):
                    if sums[n] is not None:
                        totals[n] = add(totals[n], turned(sums[n], c))
            at = edge - sign * j
            for n in range(6):
                if totals[n] is not None:
                    for r in range(ROWS):
                        diag[n, r, at : at + 1, :] += totals[n][r : r + 1, :]


def kernel(
    nx, ny,
    disp, vel, load, flags, mask,
    u_out, v_out, t_out, a_out, b_out,
    field, near, far, rim, corner, rim_send, corner_send,
    words, words_near, words_rim, words_corner, words_rim_send, words_corner_send,
    bond, bond_edge, diag,
    pool, load_buf, flag_buf,
    ring_one, ring_two,
    in_sem, send_sem, recv_sem, word_send, word_recv, sum_send, sum_recv,
):
    total, rate, force, pull = (pool.at[n] for n in range(4))
    ax = lax.axis_index("gx")
    ay = lax.axis_index("gy")
    here = {-1: (ax > 0, ay > 0), 1: (ax < nx - 1, ay < ny - 1)}

    def exists(dx, dy):
        cond = None
        if dx:
            cond = here[dx][0]
        if dy:
            other = here[dy][1]
            cond = other if cond is None else cond & other
        return cond

    def device(dx, dy):
        return {"gx": ax + dx, "gy": ay + dy}

    sides = [(dx, dy) for dx in (-1, 0, 1) for dy in (-1, 0, 1) if dx or dy]
    diagonals = [(dx, dy) for dx, dy in sides if dx and dy]

    own_rows = pl.ds(3, ROWS)
    own_cols = pl.ds(PAD, COLS)
    loads = [
        pltpu.make_async_copy(mask, words.at[:, own_rows, own_cols], in_sem.at[0]),
        pltpu.make_async_copy(vel, field.at[1, :, own_rows, own_cols], in_sem.at[1]),
        pltpu.make_async_copy(disp, field.at[0, :, own_rows, own_cols], in_sem.at[2]),
        pltpu.make_async_copy(disp, u_out, in_sem.at[3]),
        pltpu.make_async_copy(vel, v_out, in_sem.at[4]),
        pltpu.make_async_copy(load, load_buf, in_sem.at[5]),
        pltpu.make_async_copy(flags, flag_buf, in_sem.at[6]),
    ]
    for copy in loads:
        copy.start()

    zero8 = jnp.zeros((8, DEPTH), F32)

    barrier = pltpu.get_barrier_semaphore()
    for step in range(1, nx):
        pl.semaphore_signal(barrier, inc=1, device_id={"gx": lax.rem(ax + step, nx), "gy": ay})
    for step in range(1, ny):
        pl.semaphore_signal(barrier, inc=1, device_id={"gx": ax, "gy": lax.rem(ay + step, ny)})
    for dx, dy in diagonals:
        where = {"gx": lax.rem(ax + dx + nx, nx), "gy": lax.rem(ay + dy + ny, ny)}
        pl.semaphore_signal(barrier, inc=1, device_id=where)


    inner = slice(PAD, PAD + COLS)
    pads = (slice(0, PAD), slice(PAD + COLS, WIDE))
    borders = list(range(3)) + list(range(TALL - 3, TALL))

    def broken(*shape):
        return jnp.full(shape + (DEPTH,), -1, I32)

    def clear():
        def slot_clear(slot, carry):
            for part in range(3):
                for r in borders:
                    field[slot, part, r] = jnp.zeros((WIDE, DEPTH), F32)
                for r in range(3, TALL - 3):
                    for pad in pads:
                        field[slot, part, r, pad, :] = zero8
                for side in range(2):
                    for e in range(2):
                        for pad in pads:
                            near[slot, side, part, e, pad, :] = zero8
            for side in range(2):
                for at in range(7):
                    rim[slot, side, at, 0:8, :] = zero8
                    rim[slot, side, at, 16:24, :] = zero8
            return carry

        lax.fori_loop(0, SLOTS, slot_clear, 0)
        for w in range(4):
            for r in range(TALL):
                if r in borders:
                    words[w, r] = broken(WIDE)
                else:
                    for pad in pads:
                        words[w, r, pad, :] = broken(PAD)
            for side in range(2):
                for layer in range(3):
                    for pad in pads:
                        words_near[side, w, layer, pad, :] = broken(PAD)
                    words_rim[side, w, layer, 0:8, :] = broken(8)
                    words_rim[side, w, layer, 16:24, :] = broken(8)
        for side in range(2):
            @pl.when(ax == (nx - 1 if side else 0))
            def _():
                for slot in range(SLOTS):
                    far[slot, side, inner, :] = jnp.zeros((COLS, DEPTH), F32)
                    for part in range(3):
                        for e in range(2):
                            near[slot, side, part, e, inner, :] = jnp.zeros((COLS, DEPTH), F32)
                for w in range(4):
                    for layer in range(3):
                        words_near[side, w, layer, inner, :] = broken(COLS)

            @pl.when(ay == (ny - 1 if side else 0))
            def _():
                for slot in range(SLOTS):
                    for at in range(7):
                        rim[slot, side, at, 8:16, :] = zero8
                for w in range(4):
                    for layer in range(3):
                        words_rim[side, w, layer, 8:16, :] = broken(8)

    def edge_rows(dx):
        return (0, 2) if dx < 0 else (ROWS - 2, ROWS - 3)

    def halo_copies(slot, dx, dy):
        into = {-1: 1, 1: 0}
        if dx and dy:
            n = into[dx] * 2 + into[dy]
            return [(corner_send.at[slot, n], corner.at[slot, n], 6 + n)]
        if dx:
            first, third = edge_rows(dx)
            side = into[dx]
            return [
                (
                    field.at[slot, :, pl.ds(3 + first, 2), own_cols],
                    near.at[slot, side, :, :, own_cols],
                    side,
                ),
                (field.at[slot, 0, 3 + third, own_cols], far.at[slot, side, own_cols], 2 + side),
            ]
        side = into[dy]
        return [(rim_send.at[slot, side], rim.at[slot, side, :, pl.ds(8, 8)], 4 + side)]

    def spot(part, layer):
        return 6 if layer == 2 else part * 2 + layer

    def pack_rim(slot):
        for side in range(2):
            for part in range(3):
                for layer in range(3 if part == 1 else 2):
                    col = PAD + (layer if side else COLS - 1 - layer)
                    for r in range(ROWS):
                        rim_send[slot, side, spot(part, layer), r : r + 1, :] = field[
                            slot, part, 3 + r, col : col + 1, :
                        ]

    def ends(dx):
        return slice(0, 2) if dx < 0 else slice(ROWS - 2, ROWS)

    def beyond(dx):
        return slice(6, 8) if dx < 0 else slice(16, 18)

    def copy_of(slot, dx, dy, src, dst, n):
        return pltpu.make_async_remote_copy(
            src_ref=src, dst_ref=dst, send_sem=send_sem.at[lax.rem(slot, 2), n], recv_sem=recv_sem.at[slot, n],
            device_id=device(dx, dy),
        )

    along = [(0, -1), (0, 1)]
    across = [(-1, 0), (1, 0)]

    def send_all(slot, which):
        for dx, dy in which:
            @pl.when(exists(dx, dy))
            def _():
                for src, dst, n in halo_copies(slot, dx, dy):
                    copy_of(slot, dx, dy, src, dst, n).start()

    def send_rim(slot):
        send_all(slot, along)
        for dx, dy in diagonals:
            n = (1 if dx < 0 else 0) * 2 + (1 if dy < 0 else 0)
            for at in range(6):
                corner_send[slot, n, 2 * at : 2 * at + 2, :] = rim_send[slot, 1 if dy < 0 else 0, at, ends(dx), :]
        send_all(slot, diagonals)

    def halo_send(slot):
        pack_rim(slot)
        send_rim(slot)
        send_all(slot, across)

    def wait_all(slot, which):
        for dx, dy in which:
            @pl.when(exists(dx, dy))
            def _():
                for src, dst, n in halo_copies(slot, dx, dy):
                    copy_of(slot, dx, dy, src, dst, n).wait_send()
                for src, dst, n in halo_copies(slot, -dx, -dy):
                    copy_of(slot, dx, dy, src, dst, n).wait_recv()

    def wait_rim(slot):
        wait_all(slot, along + diagonals)
        for dx, dy in diagonals:
            sx, sy = (1 if dx > 0 else 0), (1 if dy > 0 else 0)

            @pl.when(exists(dx, dy))
            def _():
                for at in range(6):
                    rim[slot, sy, at, beyond(dx), :] = corner[slot, sx * 2 + sy, 2 * at : 2 * at + 2, :]

    def word_copies(dx, dy):
        into = {-1: 1, 1: 0}
        if dx and dy:
            n = into[dx] * 2 + into[dy]
            return [(words_corner_send.at[n], words_corner.at[n], 4 + n)]
        if dx:
            side = into[dx]
            first, third = edge_rows(dx)
            two, one = (pl.ds(0, 2), 2) if side else (pl.ds(1, 2), 0)
            w = third_word((3, 0, 0), side)
            return [
                (words.at[:, pl.ds(3 + first, 2), own_cols], words_near.at[side, :, two, own_cols], side),
                (words.at[w, 3 + third, own_cols], words_near.at[side, w, one, own_cols], 8 + side),
            ]
        side = into[dy]
        w = third_word((0, 3, 0), side)
        two = pl.ds(0, 2)
        return [
            (words_rim_send.at[side, :, two], words_rim.at[side, :, two, pl.ds(8, 8)], 2 + side),
            (words_rim_send.at[side, w, 2], words_rim.at[side, w, 2, pl.ds(8, 8)], 10 + side),
        ]

    def third_word(offset, side):
        if not side:
            offset = tuple(-part for part in offset)
        return (BONDS - 1 - NUMBER[offset]) // 31

    def word_copy(dx, dy, src, dst, n):
        return pltpu.make_async_remote_copy(
            src_ref=src, dst_ref=dst, send_sem=word_send.at[n], recv_sem=word_recv.at[n], device_id=device(dx, dy),
        )

    loads[0].wait()
    for side in range(2):
        for w in range(4):
            for layer in range(3):
                col = PAD + (layer if side else COLS - 1 - layer)
                for r in range(ROWS):
                    words_rim_send[side, w, layer, r : r + 1, :] = words[w, 3 + r, col : col + 1, :]
    for dx, dy in diagonals:
        n = (1 if dx < 0 else 0) * 2 + (1 if dy < 0 else 0)
        for w in range(4):
            for layer in range(2):
                at = (w * 2 + layer) * 2
                words_corner_send[n, at : at + 2, :] = words_rim_send[1 if dy < 0 else 0, w, layer, ends(dx), :]
    clear()
    build_bonds(words, bond, diag)
    pl.semaphore_wait(barrier, nx + ny + 2)
    for dx, dy in sides:
        @pl.when(exists(dx, dy))
        def _():
            for src, dst, n in word_copies(dx, dy):
                word_copy(dx, dy, src, dst, n).start()
    loads[2].wait()
    halo_send(0)

    loads[1].wait()
    halo_send(1)
    def words_wait(which):
        for dx, dy in which:
            @pl.when(exists(dx, dy))
            def _():
                for src, dst, n in word_copies(dx, dy):
                    word_copy(dx, dy, src, dst, n).wait_send()
                for src, dst, n in word_copies(-dx, -dy):
                    word_copy(dx, dy, src, dst, n).wait_recv()

    def words_across():
        words_wait(across)
        build_across(words, words_near, bond, diag)

    def words_along():
        words_wait(along + diagonals)
        for dx, dy in diagonals:
            sx, sy = (1 if dx > 0 else 0), (1 if dy > 0 else 0)

            @pl.when(exists(dx, dy))
            def _():
                for w in range(4):
                    for layer in range(2):
                        at = (w * 2 + layer) * 2
                        words_rim[sy, w, layer, beyond(dx), :] = words_corner[sx * 2 + sy, at : at + 2, :]

        build_along(words_rim_send, words_rim, bond_edge, diag)

    def sum_copy(src, dst, which, turn, where):
        return pltpu.make_async_remote_copy(
            src_ref=src, dst_ref=dst, send_sem=sum_send.at[which, lax.rem(turn, 2)], recv_sem=sum_recv.at[which, turn],
            device_id=where,
        )

    def sum_begin(turn, rows):
        slab = jnp.concatenate([jnp.sum(row, axis=0, keepdims=True) for row in rows] + [jnp.zeros((2, DEPTH), F32)], axis=0)
        each = jnp.broadcast_to(jnp.sum(slab, axis=1, keepdims=True), (8, DEPTH))
        mine = lax.broadcasted_iota(I32, (8, DEPTH), 0) == lax.broadcasted_iota(I32, (8, DEPTH), 1)
        ring_one[turn, ax] = jnp.sum(jnp.where(mine, each, 0.0), axis=0, keepdims=True)
        for step in range(1, nx):
            sum_copy(
                ring_one.at[turn, ax], ring_one.at[turn, ax], 0, turn, {"gx": lax.rem(ax + step, nx), "gy": ay}
            ).start()

    def sum_middle(turn):
        some = ring_one.at[turn, pl.ds(0, nx - 1)]
        copy = sum_copy(some, some, 0, turn, {"gx": ax, "gy": ay})
        copy.wait_recv()
        copy.wait_send()
        ring_two[turn, ay] = jnp.sum(ring_one[turn], axis=0)
        for step in range(1, ny):
            sum_copy(
                ring_two.at[turn, ay], ring_two.at[turn, ay], 1, turn, {"gx": ax, "gy": lax.rem(ay + step, ny)}
            ).start()

    def sum_end(turn):
        some = ring_two.at[turn, pl.ds(0, ny - 1)]
        copy = sum_copy(some, some, 1, turn, {"gx": ax, "gy": ay})
        copy.wait_recv()
        copy.wait_send()
        row = jnp.sum(ring_two[turn], axis=0)
        return [jnp.broadcast_to(row[:, n : n + 1], (8, DEPTH)) for n in range(6)]

    count = 3.0 * ROWS * nx * COLS * ny * DEPTH

    def damping_of(turn, alpha, beta):
        g0, g1, g2, h0, h1, h2 = sum_end(turn)
        kinetic = alpha * alpha * g0 + 2.0 * alpha * beta * g1 + beta * beta * g2
        rayleigh = -(alpha * alpha * h0 + 2.0 * alpha * beta * h1 + beta * beta * h2)
        rayleigh = jnp.maximum(rayleigh, 0.0)
        damping = 2.0 * jnp.sqrt((rayleigh / count) / (MASS * (kinetic / count + EPSILON)))
        return (2.0 - damping) / (2.0 + damping), 2.0 / (MASS * (2.0 + damping))

    def own(ref_slot, part, r, t):
        return field[ref_slot, part, 3 + r, pl.ds(PAD + 8 * t, 8), :]

    vregs = [(part, r, t) for part in range(3) for r in range(ROWS) for t in range(2)]

    def tally_pair(acc, v, t, w):
        return (acc[0] + v * v, acc[1] + v * t, acc[2] + t * t, acc[3] + v * w, acc[4] + t * w)

    def early_products():
        def body(r, acc):
            for part in range(3):
                for t in range(2):
                    at = (part, r, pl.ds(8 * t, 8), slice(None))
                    acc = tally_pair(acc, v_out[at], total[at], rate[at])
            return acc

        return lax.fori_loop(0, ROWS, body, (zero8,) * 5)

    def late_product(slot):
        def body(r, acc):
            acc = list(acc)
            for part in range(3):
                for t in range(2):
                    acc[t] = acc[t] + total[part, r, pl.ds(8 * t, 8), :] * own(slot, part, r, t)
            return tuple(acc)

        acc = lax.fori_loop(0, ROWS, body, (zero8,) * 2)
        return acc[0] + acc[1]

    def rest(slot, out, meanwhile):
        wait_all(slot, across)
        across_pass(slot, near, far, bond, out)
        meanwhile()
        wait_rim(slot)

        def put(part, r, at, value):
            out[part, r, at : at + 1, :] += value

        spread(along_terms(slot, rim, bond_edge), put)

    for copy in loads[3:]:
        copy.wait()

    def begin(n, carry):
        out = pool.at[n]
        local_pass(n, field, bond, None, out)

        @pl.when(n == 0)
        def _():
            words_across()

        def meanwhile():
            @pl.when(n == 0)
            def _():
                words_along()

        rest(n, out, meanwhile)
        loaded = lax.div(3 - n, 3).astype(F32)
        to = lax.rem(n + 2, 4)

        def put(r, carry):
            for t in range(2):
                at = (r, pl.ds(8 * t, 8), slice(None))
                active = loaded * flag_buf[at].astype(F32)
                u = [own(n, part, r, t) for part in range(3)]
                for part in range(3):
                    value = less_diagonal(out[(part,) + at], diag, part, r, t, u)
                    value = value + active * load_buf[(part,) + at]
                    out[(part,) + at] = value
                    field[to, part, 3 + r, pl.ds(PAD + 8 * t, 8), :] = value
            return carry

        lax.fori_loop(0, ROWS, put, 0)

        @pl.when(n < 3)
        def _():
            halo_send(to)

        @pl.when(n == 1)
        def _():
            sum_begin(0, early_products() + (zero8,))

        @pl.when(n == 2)
        def _():
            sum_middle(0)
            sum_begin(1, early_products() + (late_product(0),))

        return carry

    lax.fori_loop(0, 4, begin, 0)

    def advance(alpha, beta, slot):
        def body(r, acc):
            for part in range(3):
                for t in range(2):
                    at = (part, r, pl.ds(8 * t, 8), slice(None))
                    v, tt, w, y = v_out[at], total[at], rate[at], own(slot, part, r, t)
                    v = alpha * v + beta * tt
                    w = alpha * w + beta * y
                    tt = tt + w
                    v_out[at] = v
                    u_out[at] = u_out[at] + v
                    rate[at] = w
                    total[at] = tt
                    acc = tally_pair(acc, v, tt, w)
            return acc

        return lax.fori_loop(0, ROWS, body, (zero8,) * 5)

    def cycle(n, carry):
        alpha, beta = carry
        slot = lax.rem(n, 2)
        other = 1 - slot
        local_pass(slot, field, bond, diag, force)
        wait_all(slot, across)
        across_pass(slot, near, far, bond, force)
        sum_middle(n + 1)
        alpha, beta = damping_of(n, alpha, beta)

        def body(r, carry):
            for part in range(3):
                for t in range(2):
                    at = (part, r, pl.ds(8 * t, 8), slice(None))
                    x = alpha * pull[at] + beta * force[at]
                    pull[at] = x
                    field[other, part, 3 + r, pl.ds(PAD + 8 * t, 8), :] = own(slot, part, r, t) + x
            return carry

        lax.fori_loop(0, ROWS, body, 0)
        pack_rim(other)
        wait_rim(slot)
        terms = [[(part, j, beta * value) for part, j, value in found] for found in along_terms(slot, rim, bond_edge)]
        for side in range(2):
            for part, j, value in terms[side]:
                rim_send[other, 1 - side, spot(part, j)] += value
        more = n < ITERS - 3

        @pl.when(more)
        def _():
            send_rim(other)

        def put(part, r, at, value):
            pull[part, r, at : at + 1, :] += value
            field[other, part, 3 + r, PAD + at : PAD + at + 1, :] += value

        spread(terms, put)
        early = advance(alpha, beta, slot)
        sum_begin(n + 2, early + (late_product(other),))

        @pl.when(more)
        def _():
            send_all(other, across)

        return alpha, beta

    one = jnp.ones((8, DEPTH), F32)
    alpha, beta = lax.fori_loop(0, ITERS - 2, cycle, (one, jnp.zeros((8, DEPTH), F32)))
    sum_middle(ITERS - 1)
    alpha, beta = damping_of(ITERS - 2, alpha, beta)
    slot = (ITERS - 2) % 2

    def last(r, carry):
        for part in range(3):
            for t in range(2):
                at = (part, r, pl.ds(8 * t, 8), slice(None))
                v, tt = v_out[at], total[at]
                v = alpha * v + beta * tt
                v_out[at] = v
                u_out[at] = u_out[at] + v
                t_out[at] = tt + alpha * rate[at] + beta * own(slot, part, r, t)
        return carry

    lax.fori_loop(0, ROWS, last, 0)
    alpha, beta = damping_of(ITERS - 1, alpha, beta)
    for t in range(2):
        a_out[8 * t : 8 * t + 8, :] = alpha
        b_out[8 * t : 8 * t + 8, :] = beta


def on_device(nx, ny, disp, vel, load, flags, mask_bits):
    block = (3, ROWS, COLS, DEPTH)
    any_spec = pl.BlockSpec(memory_space=pl.ANY)
    vmem_spec = pl.BlockSpec(memory_space=pltpu.VMEM)
    turns = ITERS
    dma = pltpu.SemaphoreType.DMA
    scratch = [
        pltpu.VMEM((SLOTS, 3, TALL, WIDE, DEPTH), F32),
        pltpu.VMEM((SLOTS, 2, 3, 2, WIDE, DEPTH), F32),
        pltpu.VMEM((SLOTS, 2, WIDE, DEPTH), F32),
        pltpu.VMEM((SLOTS, 2, 7, 24, DEPTH), F32),
        pltpu.VMEM((SLOTS, 4, 16, DEPTH), F32),
        pltpu.VMEM((SLOTS, 2, 7, 8, DEPTH), F32),
        pltpu.VMEM((SLOTS, 4, 16, DEPTH), F32),
        pltpu.VMEM((4, TALL, WIDE, DEPTH), I32),
        pltpu.VMEM((2, 4, 3, WIDE, DEPTH), I32),
        pltpu.VMEM((2, 4, 3, 24, DEPTH), I32),
        pltpu.VMEM((4, 16, DEPTH), I32),
        pltpu.VMEM((2, 4, 3, 8, DEPTH), I32),
        pltpu.VMEM((4, 16, DEPTH), I32),
        pltpu.VMEM((BONDS, ROWS * COLS, DEPTH), F32),
        pltpu.VMEM((2, len(EDGE), ROWS, DEPTH), F32),
        pltpu.VMEM((6, ROWS, COLS, DEPTH), F32),
        pltpu.VMEM((4,) + block, F32),
        pltpu.VMEM(block, F32),
        pltpu.VMEM(block[1:], I32),
        pltpu.VMEM((turns, nx, 1, DEPTH), F32),
        pltpu.VMEM((turns, ny, 1, DEPTH), F32),
        dma((7,)),
        dma((2, 10)),
        dma((SLOTS, 10)),
        dma((12,)),
        dma((12,)),
        dma((2, 2)),
        dma((2, turns)),
    ]
    u, v, total, alpha, beta = pl.pallas_call(
        functools.partial(kernel, nx, ny),
        out_shape=[pltpu.VMEM(block, F32)] * 3 + [pltpu.VMEM(block[2:], F32)] * 2,
        in_specs=[any_spec] * 5,
        out_specs=[vmem_spec] * 5,
        scratch_shapes=scratch,
        compiler_params=pltpu.CompilerParams(
            collective_id=0, has_side_effects=True, vmem_limit_bytes=60_000_000
        ),
    )(disp, vel, load, flags, mask_bits)
    v = alpha * v + beta * total
    return u + v, v


def solution(mesh):
    split = P(None, "gx", "gy", None)
    return jax.shard_map(
        functools.partial(on_device, mesh.shape["gx"], mesh.shape["gy"]),
        mesh=mesh,
        in_specs=(split, split, split, P("gx", "gy", None), split),
        out_specs=(split, split),
        check_vma=False,
    )
```
